32 devices in a mesh: section: 4 (over y, x), dp: 8 (over z, core).
Axes of the slice: x: 2, y: 2, z: 4, core: 2. Of those that a mesh axis runs over, the one named last changes fastest.
Arguments:
- activations: bfloat16 [4, 8, 257, 1792], P('section', 'dp'), may hold values from -6 to 6
- saved: bfloat16 [4, 8, 257, 1792], P('section', 'dp'), may hold values from -6 to 6
- cotangents: bfloat16 [4, 8, 257, 1792], P('section', 'dp'), may hold values from -1.1953125 to 1.1953125
- projection: bfloat16 [4, 1792, 1792], P('section'), may hold values from -0.125 to 0.125
- section_gain: float32 [4, 1792], P('section'), may hold values from 0.5 to 1.5
- final_gain: float32 [1792], replicated, may hold values from 0.5 to 1.5
- head_weight: bfloat16 [1792, 1024], P('section'), may hold values from -0.125 to 0.125
- text_embed: bfloat16 [8, 1024], P('dp'), may hold values from -6 to 6
- labels: int32 [8], P('dp'), may hold values from 0 to 7, each once
Outputs:
- next_act: bfloat16 [4, 8, 257, 1792], P('section', 'dp')
- next_grad: bfloat16 [4, 8, 257, 1792], P('section', 'dp')
- mean_loss: float32 [4], P('section')
The draws below stay inside these ranges and needn't reach their ends.
Inputs may be any that keep to these rules, and one draw needn't show every extreme that they name: labels holds each caption index once.
All inputs are finite; a program needn't handle non-finite values.
Results may differ from the reference program's by a relative error of at most 0.0039.
Values may be sent and summed in bfloat16 or wider, within the bound.
No kernel may reach another device: no remote copies, remote signals or barrier semaphores. Data moves between devices by JAX's collectives and lax.ppermute only.
A program may use at most 64 MiB of HBM per device.

```python
import jax
import jax.numpy as jnp
from jax import lax

D = 1792
E = 1024
TOK = 257
B = 8
N_SECTION = 4


def block_scale(key, extent, split, low, high):
    def one(position, shards_of):
        draws = jax.random.uniform(jax.random.fold_in(jax.random.fold_in(key, 6), position), (shards_of,), jnp.float32, low / len(split), high / len(split))
        return jnp.repeat(jnp.exp(draws), extent[position] // shards_of).reshape((-1,) + (1,) * (len(extent) - position - 1))

    factor_of = one(*split[0])
    for cut in split[1:]:
        factor_of = factor_of * one(*cut)
    return factor_of


def noise(key, dims, width, most, cuts=(), held_as=jnp.bfloat16):
    array = width * jax.random.normal(key, dims, jnp.float32)
    if cuts:
        array = array * block_scale(key, dims, cuts, -0.22, 0.18)
    return jnp.clip(array, -most, most).astype(held_as)


def setup_inputs(seed: int = 0) -> dict:
    arg_keys = jax.random.split(jax.random.key(seed), 10)
    return {
        "activations": noise(arg_keys[0], (N_SECTION, B, TOK, D), 1.0, 6.0, ((0, 4), (1, 8))),
        "saved": noise(arg_keys[1], (N_SECTION, B, TOK, D), 1.0, 6.0, ((0, 4), (1, 8))),
        "cotangents": noise(arg_keys[2], (N_SECTION, B, TOK, D), 0.2, 1.1953125, ((0, 4), (1, 8))),
        "projection": noise(arg_keys[3], (N_SECTION, D, D), D ** -0.5, 0.125, ((0, 4),)),
        "section_gain": jnp.clip(1.0 + 0.1 * jax.random.normal(arg_keys[4], (N_SECTION, D), jnp.float32), 0.5, 1.5),
        "final_gain": jnp.clip(1.0 + 0.1 * jax.random.normal(arg_keys[5], (D,), jnp.float32), 0.5, 1.5),
        "head_weight": noise(arg_keys[6], (D, E), D ** -0.5, 0.125, ((0, 4),)),
        "text_embed": noise(arg_keys[7], (B, E), 1.0, 6.0, ((0, 8),)),
        "labels": jax.random.permutation(arg_keys[8], B).astype(jnp.int32),
    }


epsilon = 1e-06
logit_scale = 100.0

def norm_rows(values):
    centre = lax.optimization_barrier(jnp.mean(values, axis=-1, keepdims=True))
    centred = values - centre
    variance = lax.optimization_barrier(jnp.mean(centred * centred, axis=-1, keepdims=True))
    inverse = lax.rsqrt(variance + epsilon)
    return (centred * inverse, inverse)

def unit_rows(values):
    inverse = lax.rsqrt(lax.optimization_barrier(jnp.sum(values * values, axis=-1, keepdims=True)) + epsilon)
    return (values * inverse, inverse)

def forward_block(block_in, weight, scale_row):
    block_shape = block_in.shape
    standard, inverse = norm_rows(block_in.astype(jnp.float32))
    normed = (standard * scale_row).astype(jnp.bfloat16)
    mixed = jnp.dot(normed.reshape(-1, block_shape[-1]), weight, preferred_element_type=jnp.float32)
    return (block_in.astype(jnp.float32) + mixed.reshape(block_shape)).astype(jnp.bfloat16)

def backward_block(cotangent, restored, weight, scale_row):
    block_shape = restored.shape
    standard, inverse = norm_rows(restored.astype(jnp.float32))
    d_normed = lax.dot_general(cotangent.reshape(-1, block_shape[-1]), weight, (((1,), (1,)), ((), ())), preferred_element_type=jnp.float32).reshape(block_shape)
    d_standard = d_normed * scale_row
    d_input = cotangent.astype(jnp.float32) + inverse * (d_standard - lax.optimization_barrier(jnp.mean(d_standard, axis=-1, keepdims=True)) - standard * lax.optimization_barrier(jnp.mean(d_standard * standard, axis=-1, keepdims=True)))
    return d_input.astype(jnp.bfloat16)

def reference(activations, saved, cotangents, projection, section_gain, final_gain, head_weight, text_embed, labels):
    block_out = lax.map(lambda item: forward_block(item[0], item[1], item[2]), (activations, projection, section_gain))
    last_out = block_out[-1]
    pooled = lax.optimization_barrier(jnp.mean(last_out.astype(jnp.float32), axis=1))
    pooled_std, pooled_inv = norm_rows(pooled)
    pooled_norm = (pooled_std * final_gain).astype(jnp.bfloat16)
    embedding = jnp.dot(pooled_norm, head_weight, preferred_element_type=jnp.float32)
    image_unit, image_inv = unit_rows(embedding)
    text_unit, text_inv = unit_rows(text_embed.astype(jnp.float32))
    logits = logit_scale * jnp.dot(image_unit, text_unit.T, precision=lax.Precision.HIGHEST)
    count = logits.shape[0]
    targets = (labels[:, None] == jnp.arange(count, dtype=jnp.int32)[None, :]).astype(jnp.float32)
    row_lse = jax.nn.logsumexp(logits, axis=1)
    col_lse = jax.nn.logsumexp(logits, axis=0)
    picked = lax.optimization_barrier(jnp.sum(logits * targets, axis=1))
    col_picked = lax.optimization_barrier(jnp.sum(col_lse[None, :] * targets, axis=1))
    loss_value = 0.5 * jnp.mean(row_lse - picked) + 0.5 * jnp.mean(col_picked - picked)
    section_count = activations.shape[0]
    mean_loss = jnp.zeros((section_count,), jnp.float32).at[-1].set(loss_value)
    row_prob = jnp.exp(logits - row_lse[:, None])
    col_prob = jnp.exp(logits - col_lse[None, :])
    d_logits = 0.5 * (row_prob - targets + (col_prob - targets))
    d_image = logit_scale * jnp.dot(d_logits, text_unit, precision=lax.Precision.HIGHEST)
    d_embedding = (d_image - image_unit * lax.optimization_barrier(jnp.sum(d_image * image_unit, axis=-1, keepdims=True))) * image_inv
    d_pooled_norm = lax.dot_general(d_embedding.astype(jnp.bfloat16), head_weight, (((1,), (1,)), ((), ())), preferred_element_type=jnp.float32)
    d_std = d_pooled_norm * final_gain
    d_pooled = pooled_inv * (d_std - lax.optimization_barrier(jnp.mean(d_std, axis=-1, keepdims=True)) - pooled_std * lax.optimization_barrier(jnp.mean(d_std * pooled_std, axis=-1, keepdims=True)))
    loss_grad = jnp.broadcast_to((d_pooled / TOK)[:, None, :], last_out.shape).astype(jnp.bfloat16)
    d_input = lax.map(lambda item: backward_block(item[0], item[1], item[2], item[3]), (cotangents, saved, projection, section_gain))
    next_act = jnp.concatenate([jnp.zeros_like(block_out[:1]), block_out[:-1]], axis=0)
    next_grad = jnp.concatenate([d_input[1:], loss_grad[None]], axis=0)
    return (next_act, next_grad, mean_loss)
```

```python
import functools

import jax
import jax.numpy as jnp
from jax import lax
from jax.experimental import pallas as pl
from jax.experimental.pallas import tpu as pltpu
from jax.sharding import PartitionSpec as P


epsilon = 1e-06
logit_scale = 100.0
lane = 128
F32 = jnp.float32
BF16 = jnp.bfloat16


def shift_pairs(count, steps):
    first, last = (max(0, -steps), min(count, count - steps))
    return [(source, source + steps) for source in range(first, last)]


def vmem(count):
    return [pl.BlockSpec(memory_space=pltpu.VMEM)] * count


def row_stats(values):
    width = values.shape[-1]
    centre = jnp.sum(values, axis=-1, keepdims=True) * (1.0 / width)
    centred = values - centre
    variance = jnp.sum(centred * centred, axis=-1, keepdims=True) * (1.0 / width)
    return centre, centred, lax.rsqrt(variance + epsilon)


def thirds(values):
    high = values.astype(BF16).astype(F32)
    rest = values - high
    middle = rest.astype(BF16).astype(F32)
    low = (rest - middle).astype(BF16).astype(F32)
    return high, middle, low


NN = (((1,), (0,)), ((), ()))
NT = (((1,), (1,)), ((), ()))


def dot(left, right, form):
    return lax.dot_general(left, right, form, preferred_element_type=F32)


def tiles_of(depth):
    width = 256 if depth % 256 == 0 else lane
    return [(start, start + width) for start in range(0, depth, width)]


def put(outs, low, high, block):
    start = 0
    for out in outs:
        out[:, low:high] = block[start : start + out.shape[0]]
        start += out.shape[0]


def forward_kernel(act, gain, weight, pooled, *outs):
    values = act[...].astype(F32)
    _, centred, inverse = row_stats(values)
    normed = (centred * inverse * gain[...]).astype(BF16)
    for low, high in tiles_of(act.shape[1]):
        mixed = dot(normed, weight[:, low:high], NN)
        block = (act[:, low:high].astype(F32) + mixed).astype(BF16)
        put(outs, low, high, block)
        pooled[:, low:high] = jnp.sum(block.astype(F32), axis=0, keepdims=True) * (
            1.0 / act.shape[0]
        )


def limit(mib):
    return pltpu.CompilerParams(vmem_limit_bytes=mib * 2**20)


def block_cost(rows, depth):
    return pl.CostEstimate(
        flops=2 * rows * depth * depth, bytes_accessed=2 * depth * depth, transcendentals=0
    )


def forward_block(act, gain, weight, cuts):
    rows, depth = act.shape
    parts = [jax.ShapeDtypeStruct((count, depth), BF16) for count in cuts]
    return pl.pallas_call(
        forward_kernel,
        in_specs=vmem(3),
        out_specs=vmem(1 + len(cuts)),
        out_shape=[jax.ShapeDtypeStruct((1, depth), F32)] + parts,
        compiler_params=limit(20),
        cost_estimate=block_cost(rows, depth),
        name="forward_block",
    )(act, gain, weight)


def backward_kernel(cot, saved, gain, weight, *refs):
    outs, grads = refs[:-1], refs[-1]
    depth = cot.shape[1]
    centre, _, inverse = row_stats(saved[...].astype(F32))
    total, total_unit = 0.0, 0.0
    for low, high in tiles_of(depth):
        grad = dot(cot[...], weight[low:high], NT) * gain[:, low:high]
        grads[:, low:high] = grad
        total = total + jnp.sum(grad, axis=-1, keepdims=True)
        unit = (saved[:, low:high].astype(F32) - centre) * inverse
        total_unit = total_unit + jnp.sum(grad * unit, axis=-1, keepdims=True)
    mean = total * (1.0 / depth)
    mean_unit = total_unit * (1.0 / depth)
    for low, high in tiles_of(depth):
        unit = (saved[:, low:high].astype(F32) - centre) * inverse
        block = inverse * (grads[:, low:high] - mean - unit * mean_unit)
        put(outs, low, high, (cot[:, low:high].astype(F32) + block).astype(BF16))


def backward_block(cot, saved, gain, weight, cuts):
    rows, depth = cot.shape
    return pl.pallas_call(
        backward_kernel,
        in_specs=vmem(4),
        out_specs=vmem(len(cuts)),
        out_shape=[jax.ShapeDtypeStruct((count, depth), BF16) for count in cuts],
        scratch_shapes=[pltpu.VMEM((rows, depth), F32)],
        compiler_params=limit(20),
        cost_estimate=block_cost(rows, depth),
        name="backward_block",
    )(cot, saved, gain, weight)


def tail_rows(rows):
    return -(-(rows + lane) // lane)


def pack_kernel(rows, text, head, pack):
    values = text[...].astype(F32)
    unit = values * lax.rsqrt(jnp.sum(values * values, axis=-1, keepdims=True) + epsilon)
    pieces = jnp.concatenate(thirds(unit) + (jnp.zeros((5, unit.shape[1]), F32),), axis=0)
    shadow = jnp.sum(dot(pieces.astype(BF16), head[...], NT), axis=0, keepdims=True)
    count = tail_rows(rows)
    shadow = jnp.concatenate([shadow, jnp.zeros((1, count * lane - rows), F32)], axis=1)
    start = lax.rem(lax.axis_index("section") * rows, lane)
    shadow = pltpu.roll(jnp.broadcast_to(shadow, (8, count * lane)), start, 1)[0:1]
    lines = [
        part[:, lane * tile : lane * (tile + 1)] for part in thirds(shadow) for tile in range(count)
    ]
    height = pack.shape[0] - rows
    lines.append(jnp.zeros((height - len(lines), lane), F32))
    width = pack.shape[1]
    mine = pl.ds(pl.multiple_of(lax.axis_index("dp") * width, width), width)
    pack[:rows] = head[:, mine]
    pack[rows:] = jnp.concatenate(lines, axis=0).astype(BF16)


def pack_head(text, head, devices):
    rows, width = head.shape
    height = rows + -(-3 * tail_rows(rows) // 16) * 16
    return pl.pallas_call(
        functools.partial(pack_kernel, rows),
        in_specs=vmem(2),
        out_specs=pl.BlockSpec(memory_space=pltpu.VMEM),
        out_shape=jax.ShapeDtypeStruct((height, width // devices), BF16),
        compiler_params=limit(4),
        cost_estimate=pl.CostEstimate(
            flops=4 * 10**9, bytes_accessed=2 * rows * width, transcendentals=0
        ),
        name="pack_head",
    )(text, head)


def features_kernel(rows, pooled, gain, label, *refs):
    packs, (message, standard) = refs[:-2], refs[-2:]
    depth = pooled.shape[1]
    count = tail_rows(rows)
    tiles = [jnp.zeros((1, lane), F32)] * (depth // lane + count)
    for section, pack in enumerate(packs):
        tail = pack[rows:].astype(F32)
        for tile in range(count):
            place = section * rows // lane + tile
            tiles[place] = tiles[place] + sum(
                tail[part * count + tile : part * count + tile + 1] for part in range(3)
            )
    message[:, :depth] = jnp.concatenate(tiles[: depth // lane], axis=1)
    _, centred, inverse = row_stats(pooled[...])
    unit = centred * inverse
    standard[:, :depth] = unit
    standard[:, depth:] = jnp.broadcast_to(inverse, (1, lane))
    message[:, depth : 2 * depth] = (unit * gain[...]).astype(BF16).astype(F32)
    message[:, 2 * depth :] = jnp.full((1, lane), label[0], jnp.int32).astype(F32)


def features(pooled, gain, label, packs, rows):
    depth = pooled.shape[1]
    return pl.pallas_call(
        functools.partial(features_kernel, rows),
        in_specs=vmem(2) + [pl.BlockSpec(memory_space=pltpu.SMEM)] + vmem(len(packs)),
        out_specs=vmem(2),
        out_shape=[
            jax.ShapeDtypeStruct((1, 2 * depth + lane), F32),
            jax.ShapeDtypeStruct((1, depth + lane), F32),
        ],
        compiler_params=limit(4),
        name="features",
    )(pooled, gain, label, *packs)


def embed_kernel(rows, depth, table, *refs):
    packs, (keep, send, scores, column) = refs[:-4], refs[-4:]
    count = table.shape[0]
    half = count // 2
    for section, pack in enumerate(packs):
        column[section * rows : (section + 1) * rows] = pack[:rows]
    normed = table[:, depth : 2 * depth].astype(BF16)
    weight = column[...]
    embedding = dot(normed, weight, NN)
    pieces = jnp.concatenate(thirds(embedding), axis=0).astype(BF16)
    product = dot(pieces, weight, NT)
    product = product[:count] + product[count : 2 * count] + product[2 * count :]
    shadow = jnp.concatenate(thirds(table[:, :depth]), axis=0).astype(BF16)
    score = dot(normed, shadow, NT)
    score = score[:, :count] + score[:, count : 2 * count] + score[:, 2 * count :]
    scores[...] = jnp.concatenate([score, jnp.zeros((count, lane - count), F32)], axis=1)
    square = jnp.sum(embedding * embedding, axis=-1, keepdims=True)
    place = lax.broadcasted_iota(jnp.int32, (count, lane), 0)
    across = lax.broadcasted_iota(jnp.int32, (count, lane), 1)
    square = jnp.sum(jnp.where(place == across, square, 0.0), axis=0, keepdims=True)
    square = jnp.broadcast_to(square, (half, lane))
    keep[:, :depth] = product[:half]
    keep[:, depth:] = square
    send[:, :depth] = product[half:]
    send[:, depth:] = square


def embed(table, packs, rows, depth):
    count = table.shape[0]
    part = jax.ShapeDtypeStruct((count // 2, depth + lane), F32)
    return pl.pallas_call(
        functools.partial(embed_kernel, rows, depth),
        in_specs=vmem(1 + len(packs)),
        out_specs=vmem(3),
        out_shape=[part, part, jax.ShapeDtypeStruct((count, lane), F32)],
        scratch_shapes=[pltpu.VMEM((depth, packs[0].shape[1]), BF16)],
        compiler_params=limit(4),
        name="embed",
    )(table, *packs)


def swapped(square, bit):
    across = lax.broadcasted_iota(jnp.int32, square.shape, 1)
    width = square.shape[1]
    up = pltpu.roll(square, bit, 1)
    down = pltpu.roll(square, width - bit, 1)
    return jnp.where((across & bit) == 0, down, up)


def fold_kernel(bit, depth, mine, theirs, keep, send):
    half = mine.shape[0] // 2
    total = mine[:, :depth] + theirs[:, :depth]
    square = jnp.broadcast_to(mine[0:1, depth:], (8, lane)) + swapped(
        jnp.broadcast_to(theirs[0:1, depth:], (8, lane)), bit
    )
    keep[:, :depth] = total[:half]
    keep[:, depth:] = square[:half]
    send[:, :depth] = total[half:]
    send[:, depth:] = square[:half]


def fold(mine, theirs, bit, depth):
    part = jax.ShapeDtypeStruct((mine.shape[0] // 2, mine.shape[1]), F32)
    return pl.pallas_call(
        functools.partial(fold_kernel, bit, depth),
        in_specs=vmem(2),
        out_specs=vmem(2),
        out_shape=[part, part],
        compiler_params=limit(4),
        name="fold",
    )(mine, theirs)


def loss_kernel(depth, tokens, mine, theirs, scores, table, standard, gain, grad, loss):
    count = table.shape[0]
    shape = (count, lane)
    place = lax.broadcasted_iota(jnp.int32, shape, 0)
    across = lax.broadcasted_iota(jnp.int32, shape, 1)
    same = place == across
    inside = across < count
    square = jnp.broadcast_to(mine[0:1, depth:], (8, lane)) + swapped(
        jnp.broadcast_to(theirs[0:1, depth:], (8, lane)), 1
    )
    square = jnp.broadcast_to(square[0:1], shape)
    inverse = lax.rsqrt(jnp.sum(jnp.where(same, square, 0.0), axis=1, keepdims=True) + epsilon)
    logits = logit_scale * inverse * scores[...]
    owner = (across ^ lax.axis_index("dp")).astype(F32)
    targets = jnp.where(inside & (table[:, 2 * depth : 2 * depth + 1] == owner), 1.0, 0.0)
    masked = jnp.where(inside, logits, -jnp.inf)
    row_max = jnp.max(masked, axis=1, keepdims=True)
    row_lse = row_max + jnp.log(
        jnp.sum(jnp.where(inside, jnp.exp(masked - row_max), 0.0), axis=1, keepdims=True)
    )
    col_max = jnp.max(logits, axis=0, keepdims=True)
    col_lse = col_max + jnp.log(jnp.sum(jnp.exp(logits - col_max), axis=0, keepdims=True))
    picked = jnp.sum(logits * targets, axis=1, keepdims=True)
    col_picked = jnp.sum(col_lse * targets, axis=1, keepdims=True)
    value = 0.5 / count * jnp.sum((row_lse - picked) + (col_picked - picked), axis=0, keepdims=True)
    loss[...] = jnp.broadcast_to(value, loss.shape)
    row_prob = jnp.where(inside, jnp.exp(masked - row_lse), 0.0)
    col_prob = jnp.where(inside, jnp.exp(logits - col_lse), 0.0)
    d_logits = (0.5 * (row_prob - targets + (col_prob - targets)))[0:1]
    own_inverse = inverse[0:1]
    along = jnp.sum(d_logits * logits[0:1], axis=1, keepdims=True)
    weight = jnp.sum(
        jnp.where(same, jnp.broadcast_to(d_logits, shape), 0.0), axis=1, keepdims=True
    )
    d_text = jnp.sum(weight * table[:, :depth], axis=0, keepdims=True)
    product = mine[0:1, :depth] + theirs[0:1, :depth]
    d_normed = own_inverse * (logit_scale * d_text - along * own_inverse * product)
    d_unit = d_normed * gain[...]
    unit = standard[:, :depth]
    scale = 1.0 / depth
    mean = jnp.sum(d_unit, axis=1, keepdims=True) * scale
    mean_unit = jnp.sum(d_unit * unit, axis=1, keepdims=True) * scale
    grad[...] = standard[:, depth : depth + 1] * (d_unit - mean - unit * mean_unit) * (1.0 / tokens)


def loss_step(mine, theirs, scores, table, standard, gain, tokens):
    depth = gain.shape[1]
    return pl.pallas_call(
        functools.partial(loss_kernel, depth, tokens),
        in_specs=vmem(6),
        out_specs=vmem(2),
        out_shape=[
            jax.ShapeDtypeStruct((1, depth), F32),
            jax.ShapeDtypeStruct((1, lane), F32),
        ],
        compiler_params=limit(4),
        name="loss_step",
    )(mine, theirs, scores, table, standard, gain)


def swap_dp(value, bit):
    count = lax.axis_size("dp")
    return lax.ppermute(value, "dp", [(index, index ^ bit) for index in range(count)])


def finish_kernel(plan, *refs):
    parts, (grad, loss, next_act, next_grad, mean_loss, wide, sems) = refs[:-7], refs[-7:]
    sections = lax.axis_size("section")
    mine = lax.axis_index("section")
    mean_loss[...] = jnp.where(mine == sections - 1, loss[...], 0.0)
    outs = (next_act, next_grad)
    for section in range(sections):

        @pl.when(mine == section)
        def _(section=section):
            copies = []
            for target, start, sources in plan:
                if target == 1 and section == sections - 1:
                    continue
                part = parts[sources[section]]
                place = outs[target].at[pl.ds(start, part.shape[0])]
                copies.append(pltpu.make_async_copy(part, place, sems.at[len(copies)]))
            for copy in copies:
                copy.start()
            if section == sections - 1:
                wide[...] = jnp.broadcast_to(grad[...], wide.shape).astype(BF16)
                copies.append(pltpu.make_async_copy(wide, next_grad, sems.at[len(copies)]))
                copies[-1].start()
            for copy in copies:
                copy.wait()


def finish(plan, parts, grad, loss, tokens):
    depth = grad.shape[1]
    anywhere = pl.BlockSpec(memory_space=pl.ANY)
    return pl.pallas_call(
        functools.partial(finish_kernel, plan),
        in_specs=vmem(len(parts) + 2),
        out_specs=[anywhere, anywhere] + vmem(1),
        out_shape=[jax.ShapeDtypeStruct((tokens, depth), BF16)] * 2
        + [jax.ShapeDtypeStruct((1, lane), F32)],
        scratch_shapes=[
            pltpu.VMEM((tokens, depth), BF16),
            pltpu.SemaphoreType.DMA((len(plan) + 1,)),
        ],
        compiler_params=limit(12),
        name="finish",
    )(*parts, grad, loss)


def local(
    activations,
    saved,
    cotangents,
    projection,
    section_gain,
    final_gain,
    head_weight,
    text_embed,
    labels,
):
    sections = lax.axis_size("section")
    devices = lax.axis_size("dp")
    section_index = lax.axis_index("section")
    _, _, tokens, depth = activations.shape
    rows = head_weight.shape[0]
    act, kept, cot = (value.reshape(tokens, depth) for value in (activations, saved, cotangents))
    relayed = sections == 4
    first = tokens * 5 // 8 // 16 * 16
    cuts = (first, tokens - first) if relayed else (tokens,)

    pack = pack_head(text_embed, head_weight, devices)
    packs = [
        lax.ppermute(pack, "section", [(s, s ^ flip) for s in range(sections)])
        for flip in range(sections - 1, 0, -1)
    ] + [pack]
    pooled, *acts = forward_block(act, section_gain, projection[0], cuts)
    moved = [lax.ppermute(acts[0], "section", shift_pairs(sections, 1))]
    grads = backward_block(cot, kept, section_gain, projection[0], cuts)
    moved.append(lax.ppermute(grads[0], "section", shift_pairs(sections, -1)))
    plan = [(0, 0, (0,) * sections), (1, 0, (1,) * sections)]
    if relayed:
        moved.append(lax.ppermute(acts[1], "section", [(0, 1), (2, 3)]))
        moved.append(lax.ppermute(grads[1], "section", [(1, 0), (3, 2)]))
        hand = jnp.where(section_index == 1, acts[1], grads[1])
        hand = lax.ppermute(hand, "section", [(1, 3), (2, 0)])

    gain = final_gain.reshape(1, depth)
    message, standard = features(pooled, gain, labels, packs, rows)
    table = message
    bit = 1
    while bit < devices:
        other = swap_dp(table, bit)
        table = jnp.concatenate([table, other], axis=0)
        bit *= 2
    mine, send, scores = embed(table, packs, rows, depth)
    bit = devices // 2
    while bit > 1:
        other = swap_dp(send, bit)
        mine, send = fold(mine, other, bit, depth)
        bit //= 2
    other = swap_dp(send, 1)
    grad, loss = loss_step(mine, other, scores, table, standard, gain, tokens)
    if relayed:
        moved.append(lax.ppermute(hand, "section", [(3, 2), (0, 1)]))
        plan += [(0, first, (2, 2, 4, 2)), (1, first, (3, 4, 3, 3))]
    next_act, next_grad, mean_loss = finish(plan, moved, grad, loss, tokens)
    return (next_act[None, None], next_grad[None, None], mean_loss[0, 0:1])


def shifted(value, axis, steps):
    count = lax.axis_size(axis)
    first, last = (max(0, -steps), min(count, count - steps))
    return lax.ppermute(value, axis, [(source, source + steps) for source in range(first, last)])


def spread(block, axis, owner):
    block = jnp.where(lax.axis_index(axis) == owner, block, jnp.zeros_like(block))
    return lax.psum(block, axis)


def norm_rows(values):
    centre = jnp.mean(values, axis=-1, keepdims=True)
    centred = values - centre
    variance = jnp.mean(centred * centred, axis=-1, keepdims=True)
    inverse = lax.rsqrt(variance + epsilon)
    return (centred * inverse, inverse)


def unit_rows(values):
    inverse = lax.rsqrt(jnp.sum(values * values, axis=-1, keepdims=True) + epsilon)
    return (values * inverse, inverse)


def plain_forward(block_in, weight, scale_row):
    block_shape = block_in.shape
    standard, _ = norm_rows(block_in.astype(jnp.float32))
    normed = (standard * scale_row).astype(jnp.bfloat16)
    mixed = jnp.dot(normed.reshape(-1, block_shape[-1]), weight, preferred_element_type=jnp.float32)
    return (block_in.astype(jnp.float32) + mixed.reshape(block_shape)).astype(jnp.bfloat16)


def plain_backward(cotangent, restored, weight, scale_row):
    block_shape = restored.shape
    standard, inverse = norm_rows(restored.astype(jnp.float32))
    d_normed = lax.dot_general(
        cotangent.reshape(-1, block_shape[-1]),
        weight,
        (((1,), (1,)), ((), ())),
        preferred_element_type=jnp.float32,
    ).reshape(block_shape)
    d_standard = d_normed * scale_row
    d_input = cotangent.astype(jnp.float32) + inverse * (
        d_standard
        - jnp.mean(d_standard, axis=-1, keepdims=True)
        - standard * jnp.mean(d_standard * standard, axis=-1, keepdims=True)
    )
    return d_input.astype(jnp.bfloat16)


def contrastive(logits, label_values):
    count = logits.shape[0]
    targets = (label_values[:, None] == jnp.arange(count).astype(jnp.float32)[None, :]).astype(
        jnp.float32
    )
    row_lse = jax.nn.logsumexp(logits, axis=1)
    col_lse = jax.nn.logsumexp(logits, axis=0)
    picked = jnp.sum(logits * targets, axis=1)
    col_picked = jnp.sum(col_lse[None, :] * targets, axis=1)
    loss_value = 0.5 * jnp.mean(row_lse - picked) + 0.5 * jnp.mean(col_picked - picked)
    row_prob = jnp.exp(logits - row_lse[:, None])
    col_prob = jnp.exp(logits - col_lse[None, :])
    d_logits = 0.5 * (row_prob - targets + (col_prob - targets))
    return (loss_value, d_logits)


def plain_local(
    activations,
    saved,
    cotangents,
    projection,
    section_gain,
    final_gain,
    head_weight,
    text_embed,
    labels,
):
    sections = lax.axis_size("section")
    section_index = lax.axis_index("section")
    is_last = section_index == sections - 1
    weight = projection[0]
    scale_row = section_gain[0]
    incoming = activations[0]
    block_out = plain_forward(incoming, weight, scale_row)
    next_act = shifted(block_out[None], "section", 1)
    d_input = plain_backward(cotangents[0], saved[0], weight, scale_row)
    passed_grad = shifted(d_input[None], "section", -1)
    pooled = jnp.mean(block_out.astype(jnp.float32), axis=1)
    pooled_std, pooled_inv = norm_rows(pooled)
    pooled_norm = (pooled_std * final_gain).astype(jnp.bfloat16)
    shared = spread(pooled_norm, "section", sections - 1)
    row_count = head_weight.shape[0]
    my_columns = lax.dynamic_slice_in_dim(shared, section_index * row_count, row_count, 1)
    embedding = lax.psum(
        jnp.dot(my_columns, head_weight, preferred_element_type=jnp.float32), "section"
    )
    image_unit, image_inv = unit_rows(embedding)
    own_count = image_unit.shape[0]
    text_unit, _ = unit_rows(text_embed.astype(jnp.float32))
    all_image, all_text, all_labels = (
        lax.all_gather(image_unit, "dp", axis=0, tiled=True),
        lax.all_gather(text_unit, "dp", axis=0, tiled=True),
        lax.all_gather(labels.astype(jnp.float32), "dp", axis=0, tiled=True),
    )
    logits = logit_scale * jnp.dot(all_image, all_text.T, precision=lax.Precision.HIGHEST)
    loss_value, d_logits = contrastive(logits, all_labels)
    own_rows = lax.dynamic_slice_in_dim(d_logits, lax.axis_index("dp") * own_count, own_count, 0)
    d_image = logit_scale * jnp.dot(own_rows, all_text, precision=lax.Precision.HIGHEST)
    d_embedding = (
        (d_image - image_unit * jnp.sum(d_image * image_unit, axis=-1, keepdims=True)) * image_inv
    ).astype(jnp.bfloat16)
    partial_value = lax.dot_general(
        d_embedding, head_weight, (((1,), (1,)), ((), ())), preferred_element_type=jnp.float32
    )
    d_pooled_norm = lax.all_gather(partial_value, "section", axis=1, tiled=True)
    d_std = d_pooled_norm * final_gain
    d_pooled = pooled_inv * (
        d_std
        - jnp.mean(d_std, axis=-1, keepdims=True)
        - pooled_std * jnp.mean(d_std * pooled_std, axis=-1, keepdims=True)
    )
    token_count = block_out.shape[1]
    loss_grad = jnp.broadcast_to((d_pooled / token_count)[:, None, :], block_out.shape).astype(
        jnp.bfloat16
    )
    next_grad = jnp.where(is_last, loss_grad[None], passed_grad)
    mean_loss = jnp.where(is_last, loss_value, jnp.float32(0.0))[None]
    return (next_act, next_grad, mean_loss)


def fits(mesh, width):
    sections, devices = mesh.shape["section"], mesh.shape["dp"]
    powers = not (sections & (sections - 1)) and not (devices & (devices - 1))
    return powers and sections > 1 and devices > 1 and width % (devices * lane) == 0


def either(mesh, *args):
    if fits(mesh, args[7].shape[1]):
        return local(*args)
    return plain_local(*args)


def solution(mesh):
    return jax.shard_map(
        functools.partial(either, mesh),
        mesh=mesh,
        in_specs=(
            P("section", "dp", None, None),
            P("section", "dp", None, None),
            P("section", "dp", None, None),
            P("section", None, None),
            P("section", None),
            P(),
            P("section", None),
            P("dp", None),
            P("dp"),
        ),
        out_specs=(P("section", "dp", None, None), P("section", "dp", None, None), P("section")),
        check_vma=False,
    )
```

```python
import functools

import jax
import jax.numpy as jnp
from jax import lax
from jax.experimental import pallas as pl
from jax.experimental.pallas import tpu as pltpu
from jax.sharding import PartitionSpec as P


epsilon = 1e-06
logit_scale = 100.0
lane = 128
F32 = jnp.float32
BF16 = jnp.bfloat16


def vmem(count):
    return [pl.BlockSpec(memory_space=pltpu.VMEM)] * count


def row_stats(values):
    width = values.shape[-1]
    centre = jnp.sum(values, axis=-1, keepdims=True) * (1.0 / width)
    centred = values - centre
    variance = jnp.sum(centred * centred, axis=-1, keepdims=True) * (1.0 / width)
    return centre, centred, lax.rsqrt(variance + epsilon)


def thirds(values):
    high = values.astype(BF16).astype(F32)
    rest = values - high
    middle = rest.astype(BF16).astype(F32)
    low = (rest - middle).astype(BF16).astype(F32)
    return high, middle, low


NN = (((1,), (0,)), ((), ()))
NT = (((1,), (1,)), ((), ()))


def dot(left, right, form):
    return lax.dot_general(left, right, form, preferred_element_type=F32)


def tiles_of(depth):
    width = 256 if depth % 256 == 0 else lane
    return [(start, start + width) for start in range(0, depth, width)]


def limit(mib):
    return pltpu.CompilerParams(vmem_limit_bytes=mib * 2**20)


def block_cost(rows, depth):
    return pl.CostEstimate(
        flops=2 * rows * depth * depth, bytes_accessed=2 * depth * depth, transcendentals=0
    )


def forward_rows(act, gain, weight, put):
    _, centred, inverse = row_stats(act[...].astype(F32))
    normed = (centred * inverse * gain[...]).astype(BF16)
    for low, high in tiles_of(act.shape[1]):
        mixed = dot(normed, weight[:, low:high], NN)
        put(low, high, (act[:, low:high].astype(F32) + mixed).astype(BF16))


def backward_rows(cot, saved, gain, weight, grads, put):
    depth = cot.shape[1]
    centre, _, inverse = row_stats(saved[...].astype(F32))
    total, total_unit = 0.0, 0.0
    for low, high in tiles_of(depth):
        grad = dot(cot[...], weight[low:high], NT) * gain[:, low:high]
        grads[:, low:high] = grad
        total = total + jnp.sum(grad, axis=-1, keepdims=True)
        unit = (saved[:, low:high].astype(F32) - centre) * inverse
        total_unit = total_unit + jnp.sum(grad * unit, axis=-1, keepdims=True)
    mean = total * (1.0 / depth)
    mean_unit = total_unit * (1.0 / depth)
    for low, high in tiles_of(depth):
        unit = (saved[:, low:high].astype(F32) - centre) * inverse
        block = inverse * (grads[:, low:high] - mean - unit * mean_unit)
        put(low, high, (cot[:, low:high].astype(F32) + block).astype(BF16))


def tail_rows(rows):
    return -(-(rows + lane) // lane)


def pack_rows(rows):
    return rows + -(-3 * tail_rows(rows) // 16) * 16


def pack_kernel(text_hbm, head_hbm, out, text, head, sems):
    copies = [
        pltpu.make_async_copy(text_hbm, text, sems.at[0]),
        pltpu.make_async_copy(head_hbm, head, sems.at[1]),
    ]
    for copy in copies:
        copy.start()
    for copy in copies:
        copy.wait()
    rows = head.shape[0]
    values = text[...].astype(F32)
    unit = values * lax.rsqrt(jnp.sum(values * values, axis=-1, keepdims=True) + epsilon)
    pieces = jnp.concatenate(thirds(unit) + (jnp.zeros((5, unit.shape[1]), F32),), axis=0)
    shadow = jnp.sum(dot(pieces.astype(BF16), head[...], NT), axis=0, keepdims=True)
    count = tail_rows(rows)
    shadow = jnp.concatenate([shadow, jnp.zeros((1, count * lane - rows), F32)], axis=1)
    start = lax.rem(lax.axis_index("section") * rows, lane)
    shadow = pltpu.roll(jnp.broadcast_to(shadow, (8, count * lane)), start, 1)[0:1]
    lines = [
        part[:, lane * tile : lane * (tile + 1)] for part in thirds(shadow) for tile in range(count)
    ]
    height = pack_rows(rows) - rows
    lines.append(jnp.zeros((height - len(lines), lane), F32))
    mine = pl.ds(pl.multiple_of(lax.axis_index("dp") * lane, lane), lane)
    out[:rows] = head[:, mine]
    out[rows:] = jnp.concatenate(lines, axis=0).astype(BF16)


def pack_head(text, head):
    return pl.pallas_call(
        pack_kernel,
        in_specs=[pl.BlockSpec(memory_space=pl.ANY)] * 2,
        out_specs=pl.BlockSpec(memory_space=pltpu.VMEM),
        out_shape=pltpu.VMEM((pack_rows(head.shape[0]), lane), BF16),
        scratch_shapes=[
            pltpu.VMEM(text.shape, BF16),
            pltpu.VMEM(head.shape, BF16),
            pltpu.SemaphoreType.DMA((2,)),
        ],
        compiler_params=limit(4),
        cost_estimate=pl.CostEstimate(
            flops=8 * 10**9, bytes_accessed=2 * head.size, transcendentals=0
        ),
        name="pack_head",
    )(stay(text), stay(head))


def early_kernel(act, saved, cot, gain, weight, low_out, high_out, grads):
    cut = low_out.shape[0]
    section = lax.axis_index("section")

    def put(low, high, block):
        low_out[:, low:high] = block[:cut]
        high_out[:, low:high] = block[cut:]

    @pl.when(section < 2)
    def _():
        forward_rows(act, gain, weight, put)

    @pl.when(section >= 2)
    def _():
        backward_rows(cot, saved, gain, weight, grads, put)


def stay(value):
    return pltpu.with_memory_space_constraint(value, pltpu.HBM)


def early_block(low, act, saved, cot, gain, weight):
    rows, depth = act.shape
    return pl.pallas_call(
        early_kernel,
        in_specs=vmem(5),
        out_specs=vmem(2),
        out_shape=[
            pltpu.VMEM((low, depth), BF16),
            pltpu.VMEM((rows - low, depth), BF16),
        ],
        scratch_shapes=[pltpu.VMEM((rows, depth), F32)],
        compiler_params=limit(12),
        cost_estimate=block_cost(rows, depth),
        name="early_block",
    )(act, saved, cot, gain, weight)


def later_kernel(act, saved, cot, gain, weight, hand, pooled, low_out, high_out, grads):
    rows, depth = act.shape
    rest = hand.shape[0]
    cut = rows - rest
    section = lax.axis_index("section")
    low_out[cut:] = jnp.zeros((rest - cut, depth), BF16)

    def put(low, high, block):
        low_out[:cut, low:high] = block[:cut]
        high_out[:, low:high] = block[cut:]

    def pool(low, high, block):
        pooled[:, low:high] = jnp.sum(block.astype(F32), axis=0, keepdims=True) * (1.0 / rows)

    @pl.when(section < 3)
    def _():
        pooled[...] = jnp.zeros_like(pooled)

    @pl.when(jnp.logical_or(section == 0, section == 3))
    def _():
        low_out[:cut] = jnp.zeros((cut, depth), BF16)
        high_out[...] = hand[...]

    @pl.when(section == 1)
    def _():
        backward_rows(cot, saved, gain, weight, grads, put)

    @pl.when(section == 2)
    def _():
        forward_rows(act, gain, weight, put)

    @pl.when(section == 3)
    def _():
        forward_rows(act, gain, weight, pool)


def later_block(act, saved, cot, gain, weight, hand):
    rows, depth = act.shape
    return pl.pallas_call(
        later_kernel,
        in_specs=vmem(6),
        out_specs=vmem(3),
        out_shape=[
            pltpu.VMEM((1, depth), F32),
            pltpu.VMEM(hand.shape, BF16),
            pltpu.VMEM(hand.shape, BF16),
        ],
        scratch_shapes=[pltpu.VMEM((rows, depth), F32)],
        compiler_params=limit(12),
        cost_estimate=block_cost(rows, depth),
        name="later_block",
    )(act, saved, cot, gain, weight, hand)


def slots(packs, height):
    own, near, pair = packs
    return [(3, own, 0), (2, near, 0), (1, pair, 0), (0, pair, height)]


def features_kernel(pooled, gain, label, message, standard):
    depth = pooled.shape[1]
    _, centred, inverse = row_stats(pooled[...])
    unit = centred * inverse
    standard[:, :depth] = unit
    standard[:, depth:] = jnp.broadcast_to(inverse, (1, lane))
    message[:, :depth] = (unit * gain[...]).astype(BF16).astype(F32)
    message[:, depth:] = jnp.full((1, lane), label[0], jnp.int32).astype(F32)


def features(pooled, gain, label):
    depth = pooled.shape[1]
    return pl.pallas_call(
        features_kernel,
        in_specs=vmem(2) + [pl.BlockSpec(memory_space=pltpu.SMEM)],
        out_specs=vmem(2),
        out_shape=[jax.ShapeDtypeStruct((1, depth + lane), F32)] * 2,
        compiler_params=limit(4),
        name="features",
    )(pooled, gain, label)


def text_row(packs, rows, height, depth):
    count = tail_rows(rows)
    tiles = [jnp.zeros((1, lane), F32)] * (depth // lane + count)
    for section, pack, base in slots(packs, height):
        tail = pack[base + rows : base + height].astype(F32)
        for tile in range(count):
            place = section * rows // lane + tile
            tiles[place] = tiles[place] + sum(
                tail[part * count + tile : part * count + tile + 1] for part in range(3)
            )
    return jnp.concatenate(tiles[: depth // lane], axis=1)


def embed_kernel(rows, height, depth, table, *refs):
    packs, (keep, send, column) = refs[:-3], refs[-3:]
    count = table.shape[0]
    half = count // 2
    for section, pack, base in slots(packs, height):
        column[section * rows : (section + 1) * rows] = pack[base : base + rows]
    weight = column[...]
    embedding = dot(table[:, :depth].astype(BF16), weight, NN)
    pieces = jnp.concatenate(thirds(embedding), axis=0).astype(BF16)
    product = dot(pieces, weight, NT)
    product = product[:count] + product[count : 2 * count] + product[2 * count :]
    square = jnp.sum(embedding * embedding, axis=-1, keepdims=True)
    place = lax.broadcasted_iota(jnp.int32, (count, lane), 0)
    across = lax.broadcasted_iota(jnp.int32, (count, lane), 1)
    square = jnp.sum(jnp.where(place == across, square, 0.0), axis=0, keepdims=True)
    text = text_row(packs, rows, height, depth)
    for out, part in ((keep, product[:half]), (send, product[half:])):
        out[:half, :depth] = part
        out[half:, :depth] = text
        out[:, depth:] = jnp.broadcast_to(square, (half + 1, lane))


def embed(table, packs, rows):
    count, width = table.shape
    depth = width - lane
    return pl.pallas_call(
        functools.partial(embed_kernel, rows, pack_rows(rows), depth),
        in_specs=vmem(1 + len(packs)),
        out_specs=vmem(2),
        out_shape=[jax.ShapeDtypeStruct((count // 2 + 1, width), F32)] * 2,
        scratch_shapes=[pltpu.VMEM((depth, lane), BF16)],
        compiler_params=limit(4),
        name="embed",
    )(table, *packs)


def swapped(square, bit):
    across = lax.broadcasted_iota(jnp.int32, square.shape, 1)
    width = square.shape[1]
    up = pltpu.roll(square, bit, 1)
    down = pltpu.roll(square, width - bit, 1)
    return jnp.where((across & bit) == 0, down, up)


def fold_kernel(bit, depth, count, mine, theirs, keep, send):
    half = count // 2
    total = mine[:count, :depth] + theirs[:count, :depth]
    square = jnp.broadcast_to(mine[0:1, depth:], (8, lane)) + swapped(
        jnp.broadcast_to(theirs[0:1, depth:], (8, lane)), bit
    )
    texts = jnp.concatenate([mine[count:, :depth], theirs[count:, :depth]], axis=0)
    for out, part in ((keep, total[:half]), (send, total[half:])):
        out[:half, :depth] = part
        out[half:, :depth] = texts
        out[:, depth:] = square[: out.shape[0]]


def fold(mine, theirs, bit, count):
    rows, width = mine.shape
    after = jax.ShapeDtypeStruct((count // 2 + 2 * (rows - count), width), F32)
    return pl.pallas_call(
        functools.partial(fold_kernel, bit, width - lane, count),
        in_specs=vmem(2),
        out_specs=vmem(2),
        out_shape=[after, after],
        compiler_params=limit(4),
        name="fold",
    )(mine, theirs)


def text_order(count):
    order, bit = [0], count // 2
    while bit:
        order += [slot ^ bit for slot in order]
        bit //= 2
    return order


def loss_kernel(depth, tokens, mine, theirs, table, standard, gain, grad, loss):
    count = table.shape[0]
    half = count // 2
    order = text_order(count)
    found = [(mine, 1 + order.index(slot)) for slot in range(count)]
    found = [(ref, row) if row <= half else (theirs, row - half) for ref, row in found]
    texts = jnp.concatenate([ref[row : row + 1, :depth] for ref, row in found], axis=0)
    pieces = jnp.concatenate(thirds(texts), axis=0).astype(BF16)
    score = dot(table[:, :depth].astype(BF16), pieces, NT)
    score = score[:, :count] + score[:, count : 2 * count] + score[:, 2 * count :]
    scores = jnp.concatenate([score, jnp.zeros((count, lane - count), F32)], axis=1)
    shape = (count, lane)
    place = lax.broadcasted_iota(jnp.int32, shape, 0)
    across = lax.broadcasted_iota(jnp.int32, shape, 1)
    same = place == across
    inside = across < count
    square = jnp.broadcast_to(mine[0:1, depth:], (8, lane)) + swapped(
        jnp.broadcast_to(theirs[0:1, depth:], (8, lane)), 1
    )
    square = jnp.broadcast_to(square[0:1], shape)
    inverse = lax.rsqrt(jnp.sum(jnp.where(same, square, 0.0), axis=1, keepdims=True) + epsilon)
    logits = logit_scale * inverse * scores
    owner = (across ^ lax.axis_index("dp")).astype(F32)
    targets = jnp.where(inside & (table[:, depth : depth + 1] == owner), 1.0, 0.0)
    masked = jnp.where(inside, logits, -jnp.inf)
    row_max = jnp.max(masked, axis=1, keepdims=True)
    row_lse = row_max + jnp.log(
        jnp.sum(jnp.where(inside, jnp.exp(masked - row_max), 0.0), axis=1, keepdims=True)
    )
    col_max = jnp.max(logits, axis=0, keepdims=True)
    col_lse = col_max + jnp.log(jnp.sum(jnp.exp(logits - col_max), axis=0, keepdims=True))
    picked = jnp.sum(logits * targets, axis=1, keepdims=True)
    col_picked = jnp.sum(col_lse * targets, axis=1, keepdims=True)
    value = 0.5 / count * jnp.sum((row_lse - picked) + (col_picked - picked), axis=0, keepdims=True)
    loss[...] = jnp.broadcast_to(value, loss.shape)
    row_prob = jnp.where(inside, jnp.exp(masked - row_lse), 0.0)
    col_prob = jnp.where(inside, jnp.exp(logits - col_lse), 0.0)
    d_logits = (0.5 * (row_prob - targets + (col_prob - targets)))[0:1]
    own_inverse = inverse[0:1]
    along = jnp.sum(d_logits * logits[0:1], axis=1, keepdims=True)
    weight = jnp.sum(
        jnp.where(same, jnp.broadcast_to(d_logits, shape), 0.0), axis=1, keepdims=True
    )
    d_text = jnp.sum(weight * texts, axis=0, keepdims=True)
    product = mine[0:1, :depth] + theirs[0:1, :depth]
    d_normed = own_inverse * (logit_scale * d_text - along * own_inverse * product)
    d_unit = d_normed * gain[...]
    unit = standard[:, :depth]
    scale = 1.0 / depth
    mean = jnp.sum(d_unit, axis=1, keepdims=True) * scale
    mean_unit = jnp.sum(d_unit * unit, axis=1, keepdims=True) * scale
    grad[...] = standard[:, depth : depth + 1] * (d_unit - mean - unit * mean_unit) * (1.0 / tokens)


def loss_step(mine, theirs, table, standard, gain, tokens):
    depth = gain.shape[1]
    return pl.pallas_call(
        functools.partial(loss_kernel, depth, tokens),
        in_specs=vmem(5),
        out_specs=vmem(2),
        out_shape=[
            jax.ShapeDtypeStruct((1, depth), F32),
            jax.ShapeDtypeStruct((1, lane), F32),
        ],
        compiler_params=limit(4),
        name="loss_step",
    )(mine, theirs, table, standard, gain)


def choose_kernel(arrived, own, out):
    section = lax.axis_index("section")
    middle = jnp.logical_or(section == 1, section == 2)

    @pl.when(middle)
    def _():
        out[...] = own[...]

    @pl.when(jnp.logical_not(middle))
    def _():
        out[...] = arrived[...]


def near(value):
    return pltpu.with_memory_space_constraint(value, pltpu.VMEM)


def stack_kernel(first, second, out):
    rows = first.shape[0]
    out[:rows] = first[...]
    out[rows:] = second[...]


def stack(first, second):
    rows, width = first.shape
    return pl.pallas_call(
        stack_kernel,
        in_specs=vmem(2),
        out_specs=pl.BlockSpec(memory_space=pltpu.VMEM),
        out_shape=pltpu.VMEM((2 * rows, width), first.dtype),
        compiler_params=limit(4),
        name="stack",
    )(near(first), near(second))


def choose(arrived, own):
    return pl.pallas_call(
        choose_kernel,
        in_specs=vmem(2),
        out_specs=pl.BlockSpec(memory_space=pltpu.VMEM),
        out_shape=pltpu.VMEM(own.shape, BF16),
        compiler_params=limit(4),
        name="choose",
    )(near(arrived), near(own))


def put_rows(plan, parts, outs, sems, more):
    for section, moves in enumerate(plan):

        @pl.when(lax.axis_index("section") == section)
        def _(section=section, moves=moves):
            copies = []

            def copy(source, target):
                copies.append(pltpu.make_async_copy(source, target, sems.at[len(copies)]))
                copies[-1].start()

            for name, count, out, start in moves:
                copy(parts[name].at[pl.ds(0, count)], outs[out].at[pl.ds(start, count)])
            more(section, copy)
            for one in copies:
                one.wait()


def gather_kernel(plan, *refs):
    parts, (next_act, next_grad, zeros, sems) = refs[:-4], refs[-4:]

    def more(section, copy):
        if section == 0:
            zeros[...] = jnp.zeros_like(zeros)
            copy(zeros, next_act)

    put_rows(plan, parts, (next_act, next_grad), sems, more)


def gather_rows(plan, parts, tokens):
    depth = parts[0].shape[1]
    hbm = pl.BlockSpec(memory_space=pltpu.HBM)
    return pl.pallas_call(
        functools.partial(gather_kernel, plan),
        in_specs=vmem(len(parts)),
        out_specs=[hbm, hbm],
        out_shape=[pltpu.HBM((tokens, depth), BF16)] * 2,
        scratch_shapes=[pltpu.VMEM((tokens, depth), BF16), pltpu.SemaphoreType.DMA((4,))],
        compiler_params=limit(6),
        name="gather_rows",
    )(*(near(part) for part in parts))


def last_kernel(plan, *refs):
    parts, refs = refs[:2], refs[2:]
    grad, loss, _, _, next_act, next_grad, mean_loss, wide, sems = refs
    last = len(plan) - 1
    mean_loss[...] = jnp.where(lax.axis_index("section") == last, loss[...], 0.0)

    def more(section, copy):
        if section == last:
            wide[...] = jnp.broadcast_to(grad[...], wide.shape).astype(BF16)
            copy(wide, next_grad)

    put_rows(plan, parts, (next_act, next_grad), sems, more)


def last_rows(plan, parts, grad, loss, next_act, next_grad):
    hbm = pl.BlockSpec(memory_space=pltpu.HBM)
    return pl.pallas_call(
        functools.partial(last_kernel, plan),
        in_specs=vmem(4) + [hbm, hbm],
        out_specs=[hbm, hbm] + vmem(1),
        out_shape=[pltpu.HBM(next_act.shape, BF16)] * 2 + [jax.ShapeDtypeStruct((1, lane), F32)],
        input_output_aliases={4: 0, 5: 1},
        scratch_shapes=[pltpu.VMEM(next_act.shape, BF16), pltpu.SemaphoreType.DMA((4,))],
        compiler_params=limit(6),
        name="last_rows",
    )(near(parts[0]), near(parts[1]), near(grad), loss, next_act, next_grad)


def swap(value, axis, bit):
    count = lax.axis_size(axis)
    return lax.ppermute(value, axis, [(index, index ^ bit) for index in range(count)])


def local(
    activations,
    saved,
    cotangents,
    projection,
    section_gain,
    final_gain,
    head_weight,
    text_embed,
    labels,
):
    devices = lax.axis_size("dp")
    _, _, tokens, depth = activations.shape
    rows = head_weight.shape[0]
    act, kept, cot = (value.reshape(tokens, depth) for value in (activations, saved, cotangents))
    low = lane
    high = tokens - low
    weight = projection[0]

    pack = pack_head(text_embed, head_weight)
    other = swap(pack, "section", 1)
    send_one, hand = early_block(low, act, kept, cot, section_gain, weight)
    one = swap(send_one, "section", 1)
    hand_high = swap(hand, "section", 2)
    pooled, send_three, send_two = later_block(act, kept, cot, section_gain, weight, hand)
    two = swap(send_two, "section", 1)
    pair = swap(stack(pack, other), "section", 2)
    packs = (pack, other, pair)

    gain = final_gain.reshape(1, depth)
    table, standard = features(pooled, gain, labels)
    bit = 1
    while bit < devices:
        other = swap(table, "dp", bit)
        table = jnp.concatenate([table, other], axis=0)
        bit *= 2
    hand_low = swap(one, "section", 2)
    three = swap(choose(hand_high, send_three), "section", 1)
    mine, send = embed(table, packs, rows)
    bit = devices // 2
    while bit > 1:
        other = swap(send, "dp", bit)
        mine, send = fold(mine, other, bit, bit)
        bit //= 2
    other = swap(send, "dp", 1)
    grad, loss = loss_step(mine, other, table, standard, gain, tokens)
    plan = (
        ((1, high, 1, low),),
        ((0, low, 0, 0), (1, high, 0, low)),
        ((0, low, 1, 0), (1, high, 1, low)),
        ((1, high, 0, low),),
    )
    next_act, next_grad = gather_rows(plan, (one, two), tokens)
    plan = (
        ((0, low, 1, 0),),
        ((1, low, 1, 0), (0, high, 1, low)),
        ((1, low, 0, 0), (0, high, 0, low)),
        ((0, low, 0, 0),),
    )
    next_act, next_grad, mean_loss = last_rows(
        plan, (three, hand_low), grad, loss, next_act, next_grad
    )
    return (next_act[None, None], next_grad[None, None], mean_loss[0, 0:1])


def shifted(value, axis, steps):
    count = lax.axis_size(axis)
    first, last = (max(0, -steps), min(count, count - steps))
    return lax.ppermute(value, axis, [(source, source + steps) for source in range(first, last)])


def spread(block, axis, owner):
    block = jnp.where(lax.axis_index(axis) == owner, block, jnp.zeros_like(block))
    return lax.psum(block, axis)


def norm_rows(values):
    centre = jnp.mean(values, axis=-1, keepdims=True)
    centred = values - centre
    variance = jnp.mean(centred * centred, axis=-1, keepdims=True)
    inverse = lax.rsqrt(variance + epsilon)
    return (centred * inverse, inverse)


def unit_rows(values):
    inverse = lax.rsqrt(jnp.sum(values * values, axis=-1, keepdims=True) + epsilon)
    return (values * inverse, inverse)


def plain_forward(block_in, weight, scale_row):
    block_shape = block_in.shape
    standard, _ = norm_rows(block_in.astype(jnp.float32))
    normed = (standard * scale_row).astype(jnp.bfloat16)
    mixed = jnp.dot(normed.reshape(-1, block_shape[-1]), weight, preferred_element_type=jnp.float32)
    return (block_in.astype(jnp.float32) + mixed.reshape(block_shape)).astype(jnp.bfloat16)


def plain_backward(cotangent, restored, weight, scale_row):
    block_shape = restored.shape
    standard, inverse = norm_rows(restored.astype(jnp.float32))
    d_normed = lax.dot_general(
        cotangent.reshape(-1, block_shape[-1]),
        weight,
        (((1,), (1,)), ((), ())),
        preferred_element_type=jnp.float32,
    ).reshape(block_shape)
    d_standard = d_normed * scale_row
    d_input = cotangent.astype(jnp.float32) + inverse * (
        d_standard
        - jnp.mean(d_standard, axis=-1, keepdims=True)
        - standard * jnp.mean(d_standard * standard, axis=-1, keepdims=True)
    )
    return d_input.astype(jnp.bfloat16)


def contrastive(logits, label_values):
    count = logits.shape[0]
    targets = (label_values[:, None] == jnp.arange(count).astype(jnp.float32)[None, :]).astype(
        jnp.float32
    )
    row_lse = jax.nn.logsumexp(logits, axis=1)
    col_lse = jax.nn.logsumexp(logits, axis=0)
    picked = jnp.sum(logits * targets, axis=1)
    col_picked = jnp.sum(col_lse[None, :] * targets, axis=1)
    loss_value = 0.5 * jnp.mean(row_lse - picked) + 0.5 * jnp.mean(col_picked - picked)
    row_prob = jnp.exp(logits - row_lse[:, None])
    col_prob = jnp.exp(logits - col_lse[None, :])
    d_logits = 0.5 * (row_prob - targets + (col_prob - targets))
    return (loss_value, d_logits)


def plain_local(
    activations,
    saved,
    cotangents,
    projection,
    section_gain,
    final_gain,
    head_weight,
    text_embed,
    labels,
):
    sections = lax.axis_size("section")
    section_index = lax.axis_index("section")
    is_last = section_index == sections - 1
    weight = projection[0]
    scale_row = section_gain[0]
    incoming = activations[0]
    block_out = plain_forward(incoming, weight, scale_row)
    next_act = shifted(block_out[None], "section", 1)
    d_input = plain_backward(cotangents[0], saved[0], weight, scale_row)
    passed_grad = shifted(d_input[None], "section", -1)
    pooled = jnp.mean(block_out.astype(jnp.float32), axis=1)
    pooled_std, pooled_inv = norm_rows(pooled)
    pooled_norm = (pooled_std * final_gain).astype(jnp.bfloat16)
    shared = spread(pooled_norm, "section", sections - 1)
    row_count = head_weight.shape[0]
    my_columns = lax.dynamic_slice_in_dim(shared, section_index * row_count, row_count, 1)
    embedding = lax.psum(
        jnp.dot(my_columns, head_weight, preferred_element_type=jnp.float32), "section"
    )
    image_unit, image_inv = unit_rows(embedding)
    own_count = image_unit.shape[0]
    text_unit, _ = unit_rows(text_embed.astype(jnp.float32))
    all_image, all_text, all_labels = (
        lax.all_gather(image_unit, "dp", axis=0, tiled=True),
        lax.all_gather(text_unit, "dp", axis=0, tiled=True),
        lax.all_gather(labels.astype(jnp.float32), "dp", axis=0, tiled=True),
    )
    logits = logit_scale * jnp.dot(all_image, all_text.T, precision=lax.Precision.HIGHEST)
    loss_value, d_logits = contrastive(logits, all_labels)
    own_rows = lax.dynamic_slice_in_dim(d_logits, lax.axis_index("dp") * own_count, own_count, 0)
    d_image = logit_scale * jnp.dot(own_rows, all_text, precision=lax.Precision.HIGHEST)
    d_embedding = (
        (d_image - image_unit * jnp.sum(d_image * image_unit, axis=-1, keepdims=True)) * image_inv
    ).astype(jnp.bfloat16)
    partial_value = lax.dot_general(
        d_embedding, head_weight, (((1,), (1,)), ((), ())), preferred_element_type=jnp.float32
    )
    d_pooled_norm = lax.all_gather(partial_value, "section", axis=1, tiled=True)
    d_std = d_pooled_norm * final_gain
    d_pooled = pooled_inv * (
        d_std
        - jnp.mean(d_std, axis=-1, keepdims=True)
        - pooled_std * jnp.mean(d_std * pooled_std, axis=-1, keepdims=True)
    )
    token_count = block_out.shape[1]
    loss_grad = jnp.broadcast_to((d_pooled / token_count)[:, None, :], block_out.shape).astype(
        jnp.bfloat16
    )
    next_grad = jnp.where(is_last, loss_grad[None], passed_grad)
    mean_loss = jnp.where(is_last, loss_value, jnp.float32(0.0))[None]
    return (next_act, next_grad, mean_loss)


def fits(mesh, width):
    sections, devices = mesh.shape["section"], mesh.shape["dp"]
    power = devices > 1 and not (devices & (devices - 1))
    return sections == 4 and power and width == devices * lane


def either(mesh, *args):
    if fits(mesh, args[7].shape[1]):
        return local(*args)
    return plain_local(*args)


def solution(mesh):
    return jax.shard_map(
        functools.partial(either, mesh),
        mesh=mesh,
        in_specs=(
            P("section", "dp", None, None),
            P("section", "dp", None, None),
            P("section", "dp", None, None),
            P("section", None, None),
            P("section", None),
            P(),
            P("section", None),
            P("dp", None),
            P("dp"),
        ),
        out_specs=(P("section", "dp", None, None), P("section", "dp", None, None), P("section")),
        check_vma=False,
    )
```

```python
import functools

import jax
import jax.numpy as jnp
from jax import lax
from jax.experimental import pallas as pl
from jax.experimental.pallas import tpu as pltpu
from jax.sharding import PartitionSpec as P


epsilon = 1e-06
logit_scale = 100.0
lane = 128
F32 = jnp.float32
BF16 = jnp.bfloat16


def vmem(count):
    return [pl.BlockSpec(memory_space=pltpu.VMEM)] * count


def row_stats(values):
    width = values.shape[-1]
    centre = jnp.sum(values, axis=-1, keepdims=True) * (1.0 / width)
    centred = values - centre
    variance = jnp.sum(centred * centred, axis=-1, keepdims=True) * (1.0 / width)
    return centre, centred, lax.rsqrt(variance + epsilon)


def thirds(values):
    high = values.astype(BF16).astype(F32)
    rest = values - high
    middle = rest.astype(BF16).astype(F32)
    low = (rest - middle).astype(BF16).astype(F32)
    return high, middle, low


NN = (((1,), (0,)), ((), ()))
NT = (((1,), (1,)), ((), ()))


def dot(left, right, form):
    return lax.dot_general(left, right, form, preferred_element_type=F32)


def tiles_of(depth):
    width = 256 if depth % 256 == 0 else lane
    return [(start, start + width) for start in range(0, depth, width)]


def limit(mib):
    return pltpu.CompilerParams(vmem_limit_bytes=mib * 2**20)


def block_cost(rows, depth):
    return pl.CostEstimate(
        flops=2 * rows * depth * depth, bytes_accessed=2 * depth * depth, transcendentals=0
    )


def forward_rows(act, gain, weight, put):
    _, centred, inverse = row_stats(act[...].astype(F32))
    normed = (centred * inverse * gain[...]).astype(BF16)
    for low, high in tiles_of(act.shape[1]):
        mixed = dot(normed, weight[:, low:high], NN)
        put(low, high, (act[:, low:high].astype(F32) + mixed).astype(BF16))


def backward_rows(cot, saved, gain, weight, grads, put):
    depth = cot.shape[1]
    centre, _, inverse = row_stats(saved[...].astype(F32))
    total, total_unit = 0.0, 0.0
    for low, high in tiles_of(depth):
        grad = dot(cot[...], weight[low:high], NT) * gain[:, low:high]
        grads[:, low:high] = grad
        total = total + jnp.sum(grad, axis=-1, keepdims=True)
        unit = (saved[:, low:high].astype(F32) - centre) * inverse
        total_unit = total_unit + jnp.sum(grad * unit, axis=-1, keepdims=True)
    mean = total * (1.0 / depth)
    mean_unit = total_unit * (1.0 / depth)
    for low, high in tiles_of(depth):
        unit = (saved[:, low:high].astype(F32) - centre) * inverse
        block = inverse * (grads[:, low:high] - mean - unit * mean_unit)
        put(low, high, (cot[:, low:high].astype(F32) + block).astype(BF16))


def tail_rows(rows):
    return -(-(rows + lane) // lane)


def pack_rows(rows):
    return rows + -(-3 * tail_rows(rows) // 16) * 16


def pack_kernel(text_hbm, head_hbm, out, text, head, sems):
    copies = [
        pltpu.make_async_copy(text_hbm, text, sems.at[0]),
        pltpu.make_async_copy(head_hbm, head, sems.at[1]),
    ]
    for copy in copies:
        copy.start()
    for copy in copies:
        copy.wait()
    rows = head.shape[0]
    values = text[...].astype(F32)
    unit = values * lax.rsqrt(jnp.sum(values * values, axis=-1, keepdims=True) + epsilon)
    pieces = jnp.concatenate(thirds(unit) + (jnp.zeros((5, unit.shape[1]), F32),), axis=0)
    shadow = jnp.sum(dot(pieces.astype(BF16), head[...], NT), axis=0, keepdims=True)
    count = tail_rows(rows)
    shadow = jnp.concatenate([shadow, jnp.zeros((1, count * lane - rows), F32)], axis=1)
    start = lax.rem(lax.axis_index("section") * rows, lane)
    shadow = pltpu.roll(jnp.broadcast_to(shadow, (8, count * lane)), start, 1)[0:1]
    lines = [
        part[:, lane * tile : lane * (tile + 1)] for part in thirds(shadow) for tile in range(count)
    ]
    height = pack_rows(rows) - rows
    lines.append(jnp.zeros((height - len(lines), lane), F32))
    mine = pl.ds(pl.multiple_of(lax.axis_index("dp") * lane, lane), lane)
    out[:rows] = head[:, mine]
    out[rows:] = jnp.concatenate(lines, axis=0).astype(BF16)


def pack_head(text, head):
    return pl.pallas_call(
        pack_kernel,
        in_specs=[pl.BlockSpec(memory_space=pl.ANY)] * 2,
        out_specs=pl.BlockSpec(memory_space=pltpu.VMEM),
        out_shape=pltpu.VMEM((pack_rows(head.shape[0]), lane), BF16),
        scratch_shapes=[
            pltpu.VMEM(text.shape, BF16),
            pltpu.VMEM(head.shape, BF16),
            pltpu.SemaphoreType.DMA((2,)),
        ],
        compiler_params=limit(4),
        cost_estimate=pl.CostEstimate(
            flops=8 * 10**9, bytes_accessed=2 * head.size, transcendentals=0
        ),
        name="pack_head",
    )(stay(text), stay(head))


def stacked_rows(extra, depth):
    return depth + -(-extra * depth // lane // 16) * 16


def put_tiles(out, low, high, block):
    for start in range(low, high, lane):
        out[start : start + lane] = block[:, start - low : start - low + lane]


def put_lines(out, extra, depth, pieces):
    lines = [
        piece[row : row + 1, start : start + lane]
        for row in range(extra)
        for piece in pieces
        for start in range(0, piece.shape[1], lane)
    ]
    lines.append(jnp.zeros((out.shape[0] - depth - len(lines), lane), F32))
    out[depth:] = jnp.concatenate(lines, axis=0).astype(BF16)


def early_kernel(act, saved, cot, gain, weight, low_out, high_out, grads):
    rows, depth = act.shape
    section = lax.axis_index("section")

    def putter():
        pieces = []

        def put(low, high, block):
            low_out[:, low:high] = block[:lane]
            put_tiles(high_out, low, high, block[lane : 2 * lane])
            pieces.append(block[2 * lane :].astype(F32))

        return pieces, put

    @pl.when(section < 2)
    def _():
        pieces, put = putter()
        forward_rows(act, gain, weight, put)
        put_lines(high_out, rows - 2 * lane, depth, pieces)

    @pl.when(section >= 2)
    def _():
        pieces, put = putter()
        backward_rows(cot, saved, gain, weight, grads, put)
        put_lines(high_out, rows - 2 * lane, depth, pieces)


def stay(value):
    return pltpu.with_memory_space_constraint(value, pltpu.HBM)


def early_block(act, saved, cot, gain, weight):
    rows, depth = act.shape
    return pl.pallas_call(
        early_kernel,
        in_specs=vmem(5),
        out_specs=vmem(2),
        out_shape=[
            pltpu.VMEM((lane, depth), BF16),
            pltpu.VMEM((stacked_rows(rows - 2 * lane, depth), lane), BF16),
        ],
        scratch_shapes=[pltpu.VMEM((rows, depth), F32)],
        compiler_params=limit(12),
        cost_estimate=block_cost(rows, depth),
        name="early_block",
    )(act, saved, cot, gain, weight)


def later_kernel(act, saved, cot, gain, weight, hand, pooled, low_out, high_out, grads):
    rows, depth = act.shape
    section = lax.axis_index("section")
    tail = low_out.shape[0] - depth
    low_out[depth:] = jnp.zeros((tail, lane), BF16)

    def putter():
        pieces = []

        def put(low, high, block):
            put_tiles(low_out, low, high, block[:lane])
            put_tiles(high_out, low, high, block[lane : 2 * lane])
            pieces.append(block[2 * lane :].astype(F32))

        return pieces, put

    def pool(low, high, block):
        pooled[:, low:high] = jnp.sum(block.astype(F32), axis=0, keepdims=True) * (1.0 / rows)

    @pl.when(section < 3)
    def _():
        pooled[...] = jnp.zeros_like(pooled)

    @pl.when(jnp.logical_or(section == 0, section == 3))
    def _():
        low_out[:depth] = jnp.zeros((depth, lane), BF16)
        high_out[...] = hand[...]

    @pl.when(section == 1)
    def _():
        pieces, put = putter()
        backward_rows(cot, saved, gain, weight, grads, put)
        put_lines(high_out, rows - 2 * lane, depth, pieces)

    @pl.when(section == 2)
    def _():
        pieces, put = putter()
        forward_rows(act, gain, weight, put)
        put_lines(high_out, rows - 2 * lane, depth, pieces)

    @pl.when(section == 3)
    def _():
        forward_rows(act, gain, weight, pool)


def later_block(act, saved, cot, gain, weight, hand):
    rows, depth = act.shape
    return pl.pallas_call(
        later_kernel,
        in_specs=vmem(6),
        out_specs=vmem(3),
        out_shape=[
            pltpu.VMEM((1, depth), F32),
            pltpu.VMEM(hand.shape, BF16),
            pltpu.VMEM(hand.shape, BF16),
        ],
        scratch_shapes=[pltpu.VMEM((rows, depth), F32)],
        compiler_params=limit(12),
        cost_estimate=block_cost(rows, depth),
        name="later_block",
    )(act, saved, cot, gain, weight, hand)


def slots(packs, height):
    own, near, pair = packs
    return [(3, own, 0), (2, near, 0), (1, pair, 0), (0, pair, height)]


def features_kernel(pooled, gain, label, message, standard):
    depth = pooled.shape[1]
    _, centred, inverse = row_stats(pooled[...])
    unit = centred * inverse
    standard[:, :depth] = unit
    standard[:, depth:] = jnp.broadcast_to(inverse, (1, lane))
    message[:, :depth] = (unit * gain[...]).astype(BF16).astype(F32)
    message[:, depth:] = jnp.full((1, lane), label[0], jnp.int32).astype(F32)


def features(pooled, gain, label):
    depth = pooled.shape[1]
    return pl.pallas_call(
        features_kernel,
        in_specs=vmem(2) + [pl.BlockSpec(memory_space=pltpu.SMEM)],
        out_specs=vmem(2),
        out_shape=[jax.ShapeDtypeStruct((1, depth + lane), F32)] * 2,
        compiler_params=limit(4),
        name="features",
    )(pooled, gain, label)


def text_row(packs, rows, height, depth):
    count = tail_rows(rows)
    tiles = [jnp.zeros((1, lane), F32)] * (depth // lane + count)
    for section, pack, base in slots(packs, height):
        tail = pack[base + rows : base + height].astype(F32)
        for tile in range(count):
            place = section * rows // lane + tile
            tiles[place] = tiles[place] + sum(
                tail[part * count + tile : part * count + tile + 1] for part in range(3)
            )
    return jnp.concatenate(tiles[: depth // lane], axis=1)


def text_kernel(rows, height, depth, *refs):
    refs[-1][...] = text_row(refs[:-1], rows, height, depth)


def own_text(packs, rows, depth):
    return pl.pallas_call(
        functools.partial(text_kernel, rows, pack_rows(rows), depth),
        in_specs=vmem(len(packs)),
        out_specs=pl.BlockSpec(memory_space=pltpu.VMEM),
        out_shape=pltpu.VMEM((1, depth), F32),
        compiler_params=limit(4),
        name="own_text",
    )(*(near(pack) for pack in packs))


def embed_kernel(rows, height, depth, table, text, *refs):
    packs, (keep, send, column) = refs[:-3], refs[-3:]
    count = table.shape[0]
    half = count // 2
    for section, pack, base in slots(packs, height):
        column[section * rows : (section + 1) * rows] = pack[base : base + rows]
    weight = column[...]
    embedding = dot(table[:, :depth].astype(BF16), weight, NN)
    pieces = jnp.concatenate(thirds(embedding), axis=0).astype(BF16)
    product = dot(pieces, weight, NT)
    product = product[:count] + product[count : 2 * count] + product[2 * count :]
    square = jnp.sum(embedding * embedding, axis=-1, keepdims=True)
    place = lax.broadcasted_iota(jnp.int32, (count, lane), 0)
    across = lax.broadcasted_iota(jnp.int32, (count, lane), 1)
    square = jnp.sum(jnp.where(place == across, square, 0.0), axis=0, keepdims=True)
    for out, part in ((keep, product[:half]), (send, product[half:])):
        out[:half, :depth] = part
        out[half:, :depth] = text[...]
        out[:, depth:] = jnp.broadcast_to(square, (half + 1, lane))


def embed(table, text, packs, rows):
    count, width = table.shape
    depth = width - lane
    return pl.pallas_call(
        functools.partial(embed_kernel, rows, pack_rows(rows), depth),
        in_specs=vmem(2 + len(packs)),
        out_specs=vmem(2),
        out_shape=[jax.ShapeDtypeStruct((count // 2 + 1, width), F32)] * 2,
        scratch_shapes=[pltpu.VMEM((depth, lane), BF16)],
        compiler_params=limit(4),
        name="embed",
    )(table, text, *packs)


def swapped(square, bit):
    across = lax.broadcasted_iota(jnp.int32, square.shape, 1)
    width = square.shape[1]
    up = pltpu.roll(square, bit, 1)
    down = pltpu.roll(square, width - bit, 1)
    return jnp.where((across & bit) == 0, down, up)


def fold_kernel(bit, depth, count, mine, theirs, keep, send):
    half = count // 2
    total = mine[:count, :depth] + theirs[:count, :depth]
    square = jnp.broadcast_to(mine[0:1, depth:], (8, lane)) + swapped(
        jnp.broadcast_to(theirs[0:1, depth:], (8, lane)), bit
    )
    texts = jnp.concatenate([mine[count:, :depth], theirs[count:, :depth]], axis=0)
    for out, part in ((keep, total[:half]), (send, total[half:])):
        out[:half, :depth] = part
        out[half:, :depth] = texts
        out[:, depth:] = square[: out.shape[0]]


def fold(mine, theirs, bit, count):
    rows, width = mine.shape
    after = jax.ShapeDtypeStruct((count // 2 + 2 * (rows - count), width), F32)
    return pl.pallas_call(
        functools.partial(fold_kernel, bit, width - lane, count),
        in_specs=vmem(2),
        out_specs=vmem(2),
        out_shape=[after, after],
        compiler_params=limit(4),
        name="fold",
    )(mine, theirs)


def text_order(count):
    order, bit = [0], count // 2
    while bit:
        order += [slot ^ bit for slot in order]
        bit //= 2
    return order


def loss_kernel(depth, tokens, mine, theirs, table, standard, gain, grad, loss):
    count = table.shape[0]
    half = count // 2
    order = text_order(count)
    found = [(mine, 1 + order.index(slot)) for slot in range(count)]
    found = [(ref, row) if row <= half else (theirs, row - half) for ref, row in found]
    texts = jnp.concatenate([ref[row : row + 1, :depth] for ref, row in found], axis=0)
    pieces = jnp.concatenate(thirds(texts), axis=0).astype(BF16)
    score = dot(table[:, :depth].astype(BF16), pieces, NT)
    score = score[:, :count] + score[:, count : 2 * count] + score[:, 2 * count :]
    scores = jnp.concatenate([score, jnp.zeros((count, lane - count), F32)], axis=1)
    shape = (count, lane)
    place = lax.broadcasted_iota(jnp.int32, shape, 0)
    across = lax.broadcasted_iota(jnp.int32, shape, 1)
    same = place == across
    inside = across < count
    square = jnp.broadcast_to(mine[0:1, depth:], (8, lane)) + swapped(
        jnp.broadcast_to(theirs[0:1, depth:], (8, lane)), 1
    )
    square = jnp.broadcast_to(square[0:1], shape)
    inverse = lax.rsqrt(jnp.sum(jnp.where(same, square, 0.0), axis=1, keepdims=True) + epsilon)
    logits = logit_scale * inverse * scores
    owner = (across ^ lax.axis_index("dp")).astype(F32)
    targets = jnp.where(inside & (table[:, depth : depth + 1] == owner), 1.0, 0.0)
    masked = jnp.where(inside, logits, -jnp.inf)
    row_max = jnp.max(masked, axis=1, keepdims=True)
    row_lse = row_max + jnp.log(
        jnp.sum(jnp.where(inside, jnp.exp(masked - row_max), 0.0), axis=1, keepdims=True)
    )
    col_max = jnp.max(logits, axis=0, keepdims=True)
    col_lse = col_max + jnp.log(jnp.sum(jnp.exp(logits - col_max), axis=0, keepdims=True))
    picked = jnp.sum(logits * targets, axis=1, keepdims=True)
    col_picked = jnp.sum(col_lse * targets, axis=1, keepdims=True)
    value = 0.5 / count * jnp.sum((row_lse - picked) + (col_picked - picked), axis=0, keepdims=True)
    loss[...] = jnp.broadcast_to(value, loss.shape)
    row_prob = jnp.where(inside, jnp.exp(masked - row_lse), 0.0)
    col_prob = jnp.where(inside, jnp.exp(logits - col_lse), 0.0)
    d_logits = (0.5 * (row_prob - targets + (col_prob - targets)))[0:1]
    own_inverse = inverse[0:1]
    along = jnp.sum(d_logits * logits[0:1], axis=1, keepdims=True)
    weight = jnp.sum(
        jnp.where(same, jnp.broadcast_to(d_logits, shape), 0.0), axis=1, keepdims=True
    )
    d_text = jnp.sum(weight * texts, axis=0, keepdims=True)
    product = mine[0:1, :depth] + theirs[0:1, :depth]
    d_normed = own_inverse * (logit_scale * d_text - along * own_inverse * product)
    d_unit = d_normed * gain[...]
    unit = standard[:, :depth]
    scale = 1.0 / depth
    mean = jnp.sum(d_unit, axis=1, keepdims=True) * scale
    mean_unit = jnp.sum(d_unit * unit, axis=1, keepdims=True) * scale
    grad[...] = standard[:, depth : depth + 1] * (d_unit - mean - unit * mean_unit) * (1.0 / tokens)


def loss_step(mine, theirs, table, standard, gain, tokens):
    depth = gain.shape[1]
    return pl.pallas_call(
        functools.partial(loss_kernel, depth, tokens),
        in_specs=vmem(5),
        out_specs=vmem(2),
        out_shape=[
            jax.ShapeDtypeStruct((1, depth), F32),
            jax.ShapeDtypeStruct((1, lane), F32),
        ],
        compiler_params=limit(4),
        name="loss_step",
    )(mine, theirs, table, standard, gain)


def choose_kernel(arrived, own, out):
    section = lax.axis_index("section")
    middle = jnp.logical_or(section == 1, section == 2)

    @pl.when(middle)
    def _():
        out[...] = own[...]

    @pl.when(jnp.logical_not(middle))
    def _():
        out[...] = arrived[...]


def near(value):
    return pltpu.with_memory_space_constraint(value, pltpu.VMEM)


def stack_kernel(first, second, out):
    rows = first.shape[0]
    out[:rows] = first[...]
    out[rows:] = second[...]


def stack(first, second):
    rows, width = first.shape
    return pl.pallas_call(
        stack_kernel,
        in_specs=vmem(2),
        out_specs=pl.BlockSpec(memory_space=pltpu.VMEM),
        out_shape=pltpu.VMEM((2 * rows, width), first.dtype),
        compiler_params=limit(4),
        name="stack",
    )(near(first), near(second))


def choose(arrived, own):
    return pl.pallas_call(
        choose_kernel,
        in_specs=vmem(2),
        out_specs=pl.BlockSpec(memory_space=pltpu.VMEM),
        out_shape=pltpu.VMEM(own.shape, BF16),
        compiler_params=limit(4),
        name="choose",
    )(near(arrived), near(own))


def put_rows(plan, parts, outs, row, sems, more):
    tokens, depth = outs[0].shape
    extra = tokens - 2 * lane
    for section, moves in enumerate(plan):

        @pl.when(lax.axis_index("section") == section)
        def _(section=section, moves=moves):
            copies = []

            def copy(source, target):
                copies.append(pltpu.make_async_copy(source, target, sems.at[len(copies)]))
                copies[-1].start()

            for name, out, start, whole in moves:
                part, out = parts[name], outs[out]
                if part.shape == (lane, depth):
                    copy(part, out.at[pl.ds(start, lane)])
                    continue
                for place in range(0, depth, lane):
                    copy(
                        part.at[pl.ds(place, lane)],
                        out.at[pl.ds(start, lane), pl.ds(place, lane)],
                    )
                if whole:
                    lines = part[depth:].astype(F32)
                    count = depth // lane
                    line = [
                        jnp.concatenate(
                            [lines[at * count + tile : at * count + tile + 1] for tile in range(count)],
                            axis=1,
                        )
                        for at in range(extra)
                    ]
                    row[16:] = jnp.concatenate(line, axis=0).astype(BF16)
                    copy(row.at[pl.ds(16, extra)], out.at[pl.ds(start + lane, extra)])
            more(section, copy)
            for one in copies:
                one.wait()


def rows_call(kernel, plan, parts, more, tokens, depth, outs=()):
    hbm = pl.BlockSpec(memory_space=pltpu.HBM)
    count = len(parts) + len(more)
    extra = tokens - 2 * lane
    loss = [jax.ShapeDtypeStruct((1, lane), F32)] if more else []
    return pl.pallas_call(
        functools.partial(kernel, plan),
        in_specs=vmem(count) + [hbm] * len(outs),
        out_specs=[hbm, hbm] + vmem(len(loss)),
        out_shape=[pltpu.HBM((tokens, depth), BF16)] * 2 + loss,
        input_output_aliases={count + place: place for place in range(len(outs))},
        scratch_shapes=[
            pltpu.VMEM((tokens, depth), BF16),
            pltpu.VMEM((16 + extra, depth), BF16),
            pltpu.SemaphoreType.DMA((2 * depth // lane + 4,)),
        ],
        compiler_params=limit(6),
    )(*(near(part) for part in parts), *more, *outs)


def gather_kernel(plan, one, two, next_act, next_grad, wide, row, sems):
    def more(section, copy):
        if section == 0:
            wide[...] = jnp.zeros_like(wide)
            copy(wide, next_act)

    put_rows(plan, (one, two), (next_act, next_grad), row, sems, more)


def loss_rows_kernel(plan, part, grad, loss, _a, _g, next_act, next_grad, mean_loss, wide, row, sems):
    last = len(plan) - 1
    mean_loss[...] = jnp.where(lax.axis_index("section") == last, loss[...], 0.0)

    def more(section, copy):
        if section == last:
            wide[...] = jnp.broadcast_to(grad[...], wide.shape).astype(BF16)
            copy(wide, next_grad)

    put_rows(plan, (part,), (next_act, next_grad), row, sems, more)


def last_kernel(plan, part, _a, _g, next_act, next_grad, _wide, row, sems):
    put_rows(plan, (part,), (next_act, next_grad), row, sems, lambda *_: None)


def swap(value, axis, bit):
    count = lax.axis_size(axis)
    return lax.ppermute(value, axis, [(index, index ^ bit) for index in range(count)])


def local(
    activations,
    saved,
    cotangents,
    projection,
    section_gain,
    final_gain,
    head_weight,
    text_embed,
    labels,
):
    devices = lax.axis_size("dp")
    _, _, tokens, depth = activations.shape
    rows = head_weight.shape[0]
    act, kept, cot = (value.reshape(tokens, depth) for value in (activations, saved, cotangents))
    weight = projection[0]

    pack = pack_head(text_embed, head_weight)
    other = swap(pack, "section", 1)
    send_one, hand = early_block(act, kept, cot, section_gain, weight)
    one = swap(send_one, "section", 1)
    hand_high = swap(hand, "section", 2)
    pooled, send_three, send_two = later_block(act, kept, cot, section_gain, weight, hand)
    two = swap(send_two, "section", 1)
    pair = swap(stack(pack, other), "section", 2)
    packs = (pack, other, pair)
    text = own_text(packs, rows, depth)

    gain = final_gain.reshape(1, depth)
    table, standard = features(pooled, gain, labels)
    bit = 1
    while bit < devices:
        other = swap(table, "dp", bit)
        table = jnp.concatenate([table, other], axis=0)
        bit *= 2
    hand_low = swap(one, "section", 2)
    three = swap(choose(hand_high, send_three), "section", 1)
    mine, send = embed(table, text, packs, rows)
    bit = devices // 2
    while bit > 1:
        other = swap(send, "dp", bit)
        mine, send = fold(mine, other, bit, bit)
        bit //= 2
    other = swap(send, "dp", 1)
    grad, loss = loss_step(mine, other, table, standard, gain, tokens)
    plan = (
        ((1, 1, lane, True),),
        ((0, 0, 0, False), (1, 0, lane, True)),
        ((0, 1, 0, False), (1, 1, lane, True)),
        ((1, 0, lane, True),),
    )
    outs = rows_call(gather_kernel, plan, (one, two), (), tokens, depth)
    plan = ((), ((0, 1, 0, False),), ((0, 0, 0, False),), ())
    *outs, mean_loss = rows_call(
        loss_rows_kernel, plan, (hand_low,), (grad, loss), tokens, depth, outs
    )
    plan = (((0, 1, 0, False),), ((0, 1, lane, True),), ((0, 0, lane, True),), ((0, 0, 0, False),))
    next_act, next_grad = rows_call(last_kernel, plan, (three,), (), tokens, depth, outs)
    return (next_act[None, None], next_grad[None, None], mean_loss[0, 0:1])


def shifted(value, axis, steps):
    count = lax.axis_size(axis)
    first, last = (max(0, -steps), min(count, count - steps))
    return lax.ppermute(value, axis, [(source, source + steps) for source in range(first, last)])


def spread(block, axis, owner):
    block = jnp.where(lax.axis_index(axis) == owner, block, jnp.zeros_like(block))
    return lax.psum(block, axis)


def norm_rows(values):
    centre = jnp.mean(values, axis=-1, keepdims=True)
    centred = values - centre
    variance = jnp.mean(centred * centred, axis=-1, keepdims=True)
    inverse = lax.rsqrt(variance + epsilon)
    return (centred * inverse, inverse)


def unit_rows(values):
    inverse = lax.rsqrt(jnp.sum(values * values, axis=-1, keepdims=True) + epsilon)
    return (values * inverse, inverse)


def plain_forward(block_in, weight, scale_row):
    block_shape = block_in.shape
    standard, _ = norm_rows(block_in.astype(jnp.float32))
    normed = (standard * scale_row).astype(jnp.bfloat16)
    mixed = jnp.dot(normed.reshape(-1, block_shape[-1]), weight, preferred_element_type=jnp.float32)
    return (block_in.astype(jnp.float32) + mixed.reshape(block_shape)).astype(jnp.bfloat16)


def plain_backward(cotangent, restored, weight, scale_row):
    block_shape = restored.shape
    standard, inverse = norm_rows(restored.astype(jnp.float32))
    d_normed = lax.dot_general(
        cotangent.reshape(-1, block_shape[-1]),
        weight,
        (((1,), (1,)), ((), ())),
        preferred_element_type=jnp.float32,
    ).reshape(block_shape)
    d_standard = d_normed * scale_row
    d_input = cotangent.astype(jnp.float32) + inverse * (
        d_standard
        - jnp.mean(d_standard, axis=-1, keepdims=True)
        - standard * jnp.mean(d_standard * standard, axis=-1, keepdims=True)
    )
    return d_input.astype(jnp.bfloat16)


def contrastive(logits, label_values):
    count = logits.shape[0]
    targets = (label_values[:, None] == jnp.arange(count).astype(jnp.float32)[None, :]).astype(
        jnp.float32
    )
    row_lse = jax.nn.logsumexp(logits, axis=1)
    col_lse = jax.nn.logsumexp(logits, axis=0)
    picked = jnp.sum(logits * targets, axis=1)
    col_picked = jnp.sum(col_lse[None, :] * targets, axis=1)
    loss_value = 0.5 * jnp.mean(row_lse - picked) + 0.5 * jnp.mean(col_picked - picked)
    row_prob = jnp.exp(logits - row_lse[:, None])
    col_prob = jnp.exp(logits - col_lse[None, :])
    d_logits = 0.5 * (row_prob - targets + (col_prob - targets))
    return (loss_value, d_logits)


def plain_local(
    activations,
    saved,
    cotangents,
    projection,
    section_gain,
    final_gain,
    head_weight,
    text_embed,
    labels,
):
    sections = lax.axis_size("section")
    section_index = lax.axis_index("section")
    is_last = section_index == sections - 1
    weight = projection[0]
    scale_row = section_gain[0]
    incoming = activations[0]
    block_out = plain_forward(incoming, weight, scale_row)
    next_act = shifted(block_out[None], "section", 1)
    d_input = plain_backward(cotangents[0], saved[0], weight, scale_row)
    passed_grad = shifted(d_input[None], "section", -1)
    pooled = jnp.mean(block_out.astype(jnp.float32), axis=1)
    pooled_std, pooled_inv = norm_rows(pooled)
    pooled_norm = (pooled_std * final_gain).astype(jnp.bfloat16)
    shared = spread(pooled_norm, "section", sections - 1)
    row_count = head_weight.shape[0]
    my_columns = lax.dynamic_slice_in_dim(shared, section_index * row_count, row_count, 1)
    embedding = lax.psum(
        jnp.dot(my_columns, head_weight, preferred_element_type=jnp.float32), "section"
    )
    image_unit, image_inv = unit_rows(embedding)
    own_count = image_unit.shape[0]
    text_unit, _ = unit_rows(text_embed.astype(jnp.float32))
    all_image, all_text, all_labels = (
        lax.all_gather(image_unit, "dp", axis=0, tiled=True),
        lax.all_gather(text_unit, "dp", axis=0, tiled=True),
        lax.all_gather(labels.astype(jnp.float32), "dp", axis=0, tiled=True),
    )
    logits = logit_scale * jnp.dot(all_image, all_text.T, precision=lax.Precision.HIGHEST)
    loss_value, d_logits = contrastive(logits, all_labels)
    own_rows = lax.dynamic_slice_in_dim(d_logits, lax.axis_index("dp") * own_count, own_count, 0)
    d_image = logit_scale * jnp.dot(own_rows, all_text, precision=lax.Precision.HIGHEST)
    d_embedding = (
        (d_image - image_unit * jnp.sum(d_image * image_unit, axis=-1, keepdims=True)) * image_inv
    ).astype(jnp.bfloat16)
    partial_value = lax.dot_general(
        d_embedding, head_weight, (((1,), (1,)), ((), ())), preferred_element_type=jnp.float32
    )
    d_pooled_norm = lax.all_gather(partial_value, "section", axis=1, tiled=True)
    d_std = d_pooled_norm * final_gain
    d_pooled = pooled_inv * (
        d_std
        - jnp.mean(d_std, axis=-1, keepdims=True)
        - pooled_std * jnp.mean(d_std * pooled_std, axis=-1, keepdims=True)
    )
    token_count = block_out.shape[1]
    loss_grad = jnp.broadcast_to((d_pooled / token_count)[:, None, :], block_out.shape).astype(
        jnp.bfloat16
    )
    next_grad = jnp.where(is_last, loss_grad[None], passed_grad)
    mean_loss = jnp.where(is_last, loss_value, jnp.float32(0.0))[None]
    return (next_act, next_grad, mean_loss)


def fits(mesh, width, tokens):
    sections, devices = mesh.shape["section"], mesh.shape["dp"]
    power = devices > 1 and not (devices & (devices - 1))
    return sections == 4 and power and width == devices * lane and 0 < tokens - 2 * lane <= 8


def either(mesh, *args):
    if fits(mesh, args[7].shape[1], args[0].shape[2]):
        return local(*args)
    return plain_local(*args)


def solution(mesh):
    return jax.shard_map(
        functools.partial(either, mesh),
        mesh=mesh,
        in_specs=(
            P("section", "dp", None, None),
            P("section", "dp", None, None),
            P("section", "dp", None, None),
            P("section", None, None),
            P("section", None),
            P(),
            P("section", None),
            P("dp", None),
            P("dp"),
        ),
        out_specs=(P("section", "dp", None, None), P("section", "dp", None, None), P("section")),
        check_vma=False,
    )
```

```python
import functools

import jax
import jax.numpy as jnp
from jax import lax
from jax.experimental import pallas as pl
from jax.experimental.pallas import tpu as pltpu
from jax.sharding import PartitionSpec as P


epsilon = 1e-06
logit_scale = 100.0
lane = 128
F32 = jnp.float32
BF16 = jnp.bfloat16


def vmem(count):
    return [pl.BlockSpec(memory_space=pltpu.VMEM)] * count


def row_stats(values):
    width = values.shape[-1]
    centre = jnp.sum(values, axis=-1, keepdims=True) * (1.0 / width)
    centred = values - centre
    variance = jnp.sum(centred * centred, axis=-1, keepdims=True) * (1.0 / width)
    return centre, centred, lax.rsqrt(variance + epsilon)


def thirds(values):
    high = values.astype(BF16).astype(F32)
    rest = values - high
    middle = rest.astype(BF16).astype(F32)
    low = (rest - middle).astype(BF16).astype(F32)
    return high, middle, low


NN = (((1,), (0,)), ((), ()))
NT = (((1,), (1,)), ((), ()))


def dot(left, right, form):
    return lax.dot_general(left, right, form, preferred_element_type=F32)


def tiles_of(depth):
    width = 256 if depth % 256 == 0 else lane
    return [(start, start + width) for start in range(0, depth, width)]


def limit(mib):
    return pltpu.CompilerParams(vmem_limit_bytes=mib * 2**20)


def block_cost(rows, depth):
    return pl.CostEstimate(
        flops=2 * rows * depth * depth, bytes_accessed=2 * depth * depth, transcendentals=0
    )


def forward_rows(act, gain, weight, put):
    _, centred, inverse = row_stats(act[...].astype(F32))
    normed = (centred * inverse * gain[...]).astype(BF16)
    for low, high in tiles_of(act.shape[1]):
        mixed = dot(normed, weight[:, low:high], NN)
        put(low, high, (act[:, low:high].astype(F32) + mixed).astype(BF16))


def backward_rows(cot, saved, gain, weight, grads, put):
    depth = cot.shape[1]
    centre, _, inverse = row_stats(saved[...].astype(F32))
    total, total_unit = 0.0, 0.0
    for low, high in tiles_of(depth):
        grad = dot(cot[...], weight[low:high], NT) * gain[:, low:high]
        grads[:, low:high] = grad
        total = total + jnp.sum(grad, axis=-1, keepdims=True)
        centred = saved[:, low:high].astype(F32) - centre
        total_unit = total_unit + jnp.sum(grad * centred, axis=-1, keepdims=True)
    mean = inverse * total * (1.0 / depth)
    slope = inverse * (inverse * (inverse * total_unit * (1.0 / depth)))
    for low, high in tiles_of(depth):
        centred = saved[:, low:high].astype(F32) - centre
        block = (inverse * grads[:, low:high] - mean) - centred * slope
        put(low, high, (cot[:, low:high].astype(F32) + block).astype(BF16))


def tail_rows(rows):
    return -(-(rows + lane) // lane)


def pack_rows(rows):
    return rows + -(-3 * tail_rows(rows) // 16) * 16


def pack_kernel(text_hbm, head_hbm, out, text, head, sems):
    copies = [
        pltpu.make_async_copy(text_hbm, text, sems.at[0]),
        pltpu.make_async_copy(head_hbm, head, sems.at[1]),
    ]
    for copy in copies:
        copy.start()
    for copy in copies:
        copy.wait()
    rows = head.shape[0]
    values = text[...].astype(F32)
    unit = values * lax.rsqrt(jnp.sum(values * values, axis=-1, keepdims=True) + epsilon)
    pieces = jnp.concatenate(thirds(unit) + (jnp.zeros((5, unit.shape[1]), F32),), axis=0)
    shadow = jnp.sum(dot(pieces.astype(BF16), head[...], NT), axis=0, keepdims=True)
    count = tail_rows(rows)
    shadow = jnp.concatenate([shadow, jnp.zeros((1, count * lane - rows), F32)], axis=1)
    start = lax.rem(lax.axis_index("section") * rows, lane)
    shadow = pltpu.roll(jnp.broadcast_to(shadow, (8, count * lane)), start, 1)[0:1]
    lines = [
        part[:, lane * tile : lane * (tile + 1)] for part in thirds(shadow) for tile in range(count)
    ]
    height = pack_rows(rows) - rows
    lines.append(jnp.zeros((height - len(lines), lane), F32))
    mine = pl.ds(pl.multiple_of(lax.axis_index("dp") * lane, lane), lane)
    out[:rows] = head[:, mine]
    out[rows:] = jnp.concatenate(lines, axis=0).astype(BF16)


def pack_head(text, head):
    return pl.pallas_call(
        pack_kernel,
        in_specs=[pl.BlockSpec(memory_space=pl.ANY)] * 2,
        out_specs=pl.BlockSpec(memory_space=pltpu.VMEM),
        out_shape=pltpu.VMEM((pack_rows(head.shape[0]), lane), BF16),
        scratch_shapes=[
            pltpu.VMEM(text.shape, BF16),
            pltpu.VMEM(head.shape, BF16),
            pltpu.SemaphoreType.DMA((2,)),
        ],
        compiler_params=limit(4),
        cost_estimate=pl.CostEstimate(
            flops=8 * 10**9, bytes_accessed=2 * head.size, transcendentals=0
        ),
        name="pack_head",
    )(stay(text), stay(head))


def stacked_rows(extra, depth):
    return depth + -(-extra * depth // lane // 16) * 16


def put_tiles(out, low, high, block):
    for start in range(low, high, lane):
        out[start : start + lane] = block[:, start - low : start - low + lane]


def put_lines(out, extra, depth, pieces):
    lines = [
        piece[row : row + 1, start : start + lane]
        for row in range(extra)
        for piece in pieces
        for start in range(0, piece.shape[1], lane)
    ]
    lines.append(jnp.zeros((out.shape[0] - depth - len(lines), lane), F32))
    out[depth:] = jnp.concatenate(lines, axis=0).astype(BF16)


def early_kernel(act, saved, cot, gain, weight, low_out, high_out, grads):
    rows, depth = act.shape
    section = lax.axis_index("section")

    def putter():
        pieces = []

        def put(low, high, block):
            low_out[:, low:high] = block[:lane]
            put_tiles(high_out, low, high, block[lane : 2 * lane])
            pieces.append(block[2 * lane :].astype(F32))

        return pieces, put

    @pl.when(section < 2)
    def _():
        pieces, put = putter()
        forward_rows(act, gain, weight, put)
        put_lines(high_out, rows - 2 * lane, depth, pieces)

    @pl.when(section >= 2)
    def _():
        pieces, put = putter()
        backward_rows(cot, saved, gain, weight, grads, put)
        put_lines(high_out, rows - 2 * lane, depth, pieces)


def stay(value):
    return pltpu.with_memory_space_constraint(value, pltpu.HBM)


def early_block(act, saved, cot, gain, weight):
    rows, depth = act.shape
    return pl.pallas_call(
        early_kernel,
        in_specs=vmem(5),
        out_specs=vmem(2),
        out_shape=[
            pltpu.VMEM((lane, depth), BF16),
            pltpu.VMEM((stacked_rows(rows - 2 * lane, depth), lane), BF16),
        ],
        scratch_shapes=[pltpu.VMEM((rows, depth), F32)],
        compiler_params=limit(12),
        cost_estimate=block_cost(rows, depth),
        name="early_block",
    )(act, saved, cot, gain, weight)


def later_kernel(act, saved, cot, gain, weight, hand, pooled, low_out, high_out, grads):
    rows, depth = act.shape
    section = lax.axis_index("section")
    tail = low_out.shape[0] - depth
    low_out[depth:] = jnp.zeros((tail, lane), BF16)

    def putter():
        pieces = []

        def put(low, high, block):
            put_tiles(low_out, low, high, block[:lane])
            put_tiles(high_out, low, high, block[lane : 2 * lane])
            pieces.append(block[2 * lane :].astype(F32))

        return pieces, put

    def pool(low, high, block):
        pooled[:, low:high] = jnp.sum(block.astype(F32), axis=0, keepdims=True) * (1.0 / rows)

    @pl.when(section < 3)
    def _():
        pooled[...] = jnp.zeros_like(pooled)

    @pl.when(jnp.logical_or(section == 0, section == 3))
    def _():
        low_out[:depth] = jnp.zeros((depth, lane), BF16)
        high_out[...] = hand[...]

    @pl.when(section == 1)
    def _():
        pieces, put = putter()
        backward_rows(cot, saved, gain, weight, grads, put)
        put_lines(high_out, rows - 2 * lane, depth, pieces)

    @pl.when(section == 2)
    def _():
        pieces, put = putter()
        forward_rows(act, gain, weight, put)
        put_lines(high_out, rows - 2 * lane, depth, pieces)

    @pl.when(section == 3)
    def _():
        forward_rows(act, gain, weight, pool)


def later_block(act, saved, cot, gain, weight, hand):
    rows, depth = act.shape
    return pl.pallas_call(
        later_kernel,
        in_specs=vmem(6),
        out_specs=vmem(3),
        out_shape=[
            pltpu.VMEM((1, depth), F32),
            pltpu.VMEM(hand.shape, BF16),
            pltpu.VMEM(hand.shape, BF16),
        ],
        scratch_shapes=[pltpu.VMEM((rows, depth), F32)],
        compiler_params=limit(12),
        cost_estimate=block_cost(rows, depth),
        name="later_block",
    )(act, saved, cot, gain, weight, hand)


def slots(packs, height):
    own, near, pair = packs
    return [(3, own, 0), (2, near, 0), (1, pair, 0), (0, pair, height)]


def features_kernel(pooled, gain, label, message, standard):
    depth = pooled.shape[1]
    _, centred, inverse = row_stats(pooled[...])
    unit = centred * inverse
    standard[:, :depth] = unit
    standard[:, depth:] = jnp.broadcast_to(inverse, (1, lane))
    message[:, :depth] = (unit * gain[...]).astype(BF16).astype(F32)
    message[:, depth:] = jnp.full((1, lane), label[0], jnp.int32).astype(F32)


def features(pooled, gain, label):
    depth = pooled.shape[1]
    return pl.pallas_call(
        features_kernel,
        in_specs=vmem(2) + [pl.BlockSpec(memory_space=pltpu.SMEM)],
        out_specs=vmem(2),
        out_shape=[jax.ShapeDtypeStruct((1, depth + lane), F32)] * 2,
        compiler_params=limit(4),
        name="features",
    )(pooled, gain, label)


def text_row(packs, rows, height, depth):
    count = tail_rows(rows)
    tiles = [jnp.zeros((1, lane), F32)] * (depth // lane + count)
    for section, pack, base in slots(packs, height):
        tail = pack[base + rows : base + height].astype(F32)
        for tile in range(count):
            place = section * rows // lane + tile
            tiles[place] = tiles[place] + sum(
                tail[part * count + tile : part * count + tile + 1] for part in range(3)
            )
    return jnp.concatenate(tiles[: depth // lane], axis=1)


def text_kernel(rows, height, depth, *refs):
    refs[-1][...] = text_row(refs[:-1], rows, height, depth)


def own_text(packs, rows, depth):
    return pl.pallas_call(
        functools.partial(text_kernel, rows, pack_rows(rows), depth),
        in_specs=vmem(len(packs)),
        out_specs=pl.BlockSpec(memory_space=pltpu.VMEM),
        out_shape=pltpu.VMEM((1, depth), F32),
        compiler_params=limit(4),
        name="own_text",
    )(*(near(pack) for pack in packs))


def embed_kernel(rows, height, depth, table, text, *refs):
    packs, (keep, send, column) = refs[:-3], refs[-3:]
    count = table.shape[0]
    half = count // 2
    for section, pack, base in slots(packs, height):
        column[section * rows : (section + 1) * rows] = pack[base : base + rows]
    weight = column[...]
    embedding = dot(table[:, :depth].astype(BF16), weight, NN)
    pieces = jnp.concatenate(thirds(embedding), axis=0).astype(BF16)
    product = dot(pieces, weight, NT)
    product = product[:count] + product[count : 2 * count] + product[2 * count :]
    square = jnp.sum(embedding * embedding, axis=-1, keepdims=True)
    place = lax.broadcasted_iota(jnp.int32, (count, lane), 0)
    across = lax.broadcasted_iota(jnp.int32, (count, lane), 1)
    square = jnp.sum(jnp.where(place == across, square, 0.0), axis=0, keepdims=True)
    for out, part in ((keep, product[:half]), (send, product[half:])):
        out[:half, :depth] = part
        out[half:, :depth] = text[...]
        out[:, depth:] = jnp.broadcast_to(square, (half + 1, lane))


def embed(table, text, packs, rows):
    count, width = table.shape
    depth = width - lane
    return pl.pallas_call(
        functools.partial(embed_kernel, rows, pack_rows(rows), depth),
        in_specs=vmem(2 + len(packs)),
        out_specs=vmem(2),
        out_shape=[jax.ShapeDtypeStruct((count // 2 + 1, width), F32)] * 2,
        scratch_shapes=[pltpu.VMEM((depth, lane), BF16)],
        compiler_params=limit(4),
        name="embed",
    )(table, text, *packs)


def swapped(square, bit):
    across = lax.broadcasted_iota(jnp.int32, square.shape, 1)
    width = square.shape[1]
    up = pltpu.roll(square, bit, 1)
    down = pltpu.roll(square, width - bit, 1)
    return jnp.where((across & bit) == 0, down, up)


def fold_kernel(bit, depth, count, mine, theirs, keep, send):
    half = count // 2
    total = mine[:count, :depth] + theirs[:count, :depth]
    square = jnp.broadcast_to(mine[0:1, depth:], (8, lane)) + swapped(
        jnp.broadcast_to(theirs[0:1, depth:], (8, lane)), bit
    )
    texts = jnp.concatenate([mine[count:, :depth], theirs[count:, :depth]], axis=0)
    for out, part in ((keep, total[:half]), (send, total[half:])):
        out[:half, :depth] = part
        out[half:, :depth] = texts
        out[:, depth:] = square[: out.shape[0]]


def fold(mine, theirs, bit, count):
    rows, width = mine.shape
    after = jax.ShapeDtypeStruct((count // 2 + 2 * (rows - count), width), F32)
    return pl.pallas_call(
        functools.partial(fold_kernel, bit, width - lane, count),
        in_specs=vmem(2),
        out_specs=vmem(2),
        out_shape=[after, after],
        compiler_params=limit(4),
        name="fold",
    )(mine, theirs)


def text_order(count):
    order, bit = [0], count // 2
    while bit:
        order += [slot ^ bit for slot in order]
        bit //= 2
    return order


def loss_kernel(depth, tokens, mine, theirs, table, standard, gain, grad, loss):
    count = table.shape[0]
    half = count // 2
    order = text_order(count)
    found = [(mine, 1 + order.index(slot)) for slot in range(count)]
    found = [(ref, row) if row <= half else (theirs, row - half) for ref, row in found]
    texts = jnp.concatenate([ref[row : row + 1, :depth] for ref, row in found], axis=0)
    pieces = jnp.concatenate(thirds(texts), axis=0).astype(BF16)
    score = dot(table[:, :depth].astype(BF16), pieces, NT)
    score = score[:, :count] + score[:, count : 2 * count] + score[:, 2 * count :]
    scores = jnp.concatenate([score, jnp.zeros((count, lane - count), F32)], axis=1)
    shape = (count, lane)
    place = lax.broadcasted_iota(jnp.int32, shape, 0)
    across = lax.broadcasted_iota(jnp.int32, shape, 1)
    same = place == across
    inside = across < count
    square = jnp.broadcast_to(mine[0:1, depth:], (8, lane)) + swapped(
        jnp.broadcast_to(theirs[0:1, depth:], (8, lane)), 1
    )
    square = jnp.broadcast_to(square[0:1], shape)
    inverse = lax.rsqrt(jnp.sum(jnp.where(same, square, 0.0), axis=1, keepdims=True) + epsilon)
    logits = logit_scale * inverse * scores
    owner = (across ^ lax.axis_index("dp")).astype(F32)
    targets = jnp.where(inside & (table[:, depth : depth + 1] == owner), 1.0, 0.0)
    masked = jnp.where(inside, logits, -jnp.inf)
    row_max = jnp.max(masked, axis=1, keepdims=True)
    row_lse = row_max + jnp.log(
        jnp.sum(jnp.where(inside, jnp.exp(masked - row_max), 0.0), axis=1, keepdims=True)
    )
    col_max = jnp.max(logits, axis=0, keepdims=True)
    col_lse = col_max + jnp.log(jnp.sum(jnp.exp(logits - col_max), axis=0, keepdims=True))
    picked = jnp.sum(logits * targets, axis=1, keepdims=True)
    col_picked = jnp.sum(col_lse * targets, axis=1, keepdims=True)
    value = 0.5 / count * jnp.sum((row_lse - picked) + (col_picked - picked), axis=0, keepdims=True)
    loss[...] = jnp.broadcast_to(value, loss.shape)
    row_prob = jnp.where(inside, jnp.exp(masked - row_lse), 0.0)
    col_prob = jnp.where(inside, jnp.exp(logits - col_lse), 0.0)
    d_logits = (0.5 * (row_prob - targets + (col_prob - targets)))[0:1]
    own_inverse = inverse[0:1]
    along = jnp.sum(d_logits * logits[0:1], axis=1, keepdims=True)
    weight = jnp.sum(
        jnp.where(same, jnp.broadcast_to(d_logits, shape), 0.0), axis=1, keepdims=True
    )
    d_text = jnp.sum(weight * texts, axis=0, keepdims=True)
    product = mine[0:1, :depth] + theirs[0:1, :depth]
    d_normed = own_inverse * (logit_scale * d_text - along * own_inverse * product)
    d_unit = d_normed * gain[...]
    unit = standard[:, :depth]
    scale = 1.0 / depth
    mean = jnp.sum(d_unit, axis=1, keepdims=True) * scale
    mean_unit = jnp.sum(d_unit * unit, axis=1, keepdims=True) * scale
    grad[...] = standard[:, depth : depth + 1] * (d_unit - mean - unit * mean_unit) * (1.0 / tokens)


def loss_step(mine, theirs, table, standard, gain, tokens):
    depth = gain.shape[1]
    return pl.pallas_call(
        functools.partial(loss_kernel, depth, tokens),
        in_specs=vmem(5),
        out_specs=vmem(2),
        out_shape=[
            jax.ShapeDtypeStruct((1, depth), F32),
            jax.ShapeDtypeStruct((1, lane), F32),
        ],
        compiler_params=limit(4),
        name="loss_step",
    )(mine, theirs, table, standard, gain)


def choose_kernel(arrived, own, out):
    section = lax.axis_index("section")
    middle = jnp.logical_or(section == 1, section == 2)

    @pl.when(middle)
    def _():
        out[...] = own[...]

    @pl.when(jnp.logical_not(middle))
    def _():
        out[...] = arrived[...]


def near(value):
    return pltpu.with_memory_space_constraint(value, pltpu.VMEM)


def stack_kernel(first, second, out):
    rows = first.shape[0]
    out[:rows] = first[...]
    out[rows:] = second[...]


def stack(first, second):
    rows, width = first.shape
    return pl.pallas_call(
        stack_kernel,
        in_specs=vmem(2),
        out_specs=pl.BlockSpec(memory_space=pltpu.VMEM),
        out_shape=pltpu.VMEM((2 * rows, width), first.dtype),
        compiler_params=limit(4),
        name="stack",
    )(near(first), near(second))


def choose(arrived, own):
    return pl.pallas_call(
        choose_kernel,
        in_specs=vmem(2),
        out_specs=pl.BlockSpec(memory_space=pltpu.VMEM),
        out_shape=pltpu.VMEM(own.shape, BF16),
        compiler_params=limit(4),
        name="choose",
    )(near(arrived), near(own))


def put_rows(plan, parts, outs, row, sems, more):
    tokens, depth = outs[0].shape
    extra = tokens - 2 * lane
    for section, moves in enumerate(plan):

        @pl.when(lax.axis_index("section") == section)
        def _(section=section, moves=moves):
            copies = []

            def copy(source, target):
                copies.append(pltpu.make_async_copy(source, target, sems.at[len(copies)]))
                copies[-1].start()

            for name, out, start, whole in moves:
                part, out = parts[name], outs[out]
                if part.shape == (lane, depth):
                    copy(part, out.at[pl.ds(start, lane)])
                    continue
                for place in range(0, depth, lane):
                    copy(
                        part.at[pl.ds(place, lane)],
                        out.at[pl.ds(start, lane), pl.ds(place, lane)],
                    )
                if whole:
                    lines = part[depth:].astype(F32)
                    count = depth // lane
                    line = [
                        jnp.concatenate(
                            [lines[at * count + tile : at * count + tile + 1] for tile in range(count)],
                            axis=1,
                        )
                        for at in range(extra)
                    ]
                    row[16:] = jnp.concatenate(line, axis=0).astype(BF16)
                    copy(row.at[pl.ds(16, extra)], out.at[pl.ds(start + lane, extra)])
            more(section, copy)
            for one in copies:
                one.wait()


def rows_call(kernel, plan, parts, more, tokens, depth, outs=()):
    hbm = pl.BlockSpec(memory_space=pltpu.HBM)
    count = len(parts) + len(more)
    extra = tokens - 2 * lane
    loss = [jax.ShapeDtypeStruct((1, lane), F32)] if more else []
    return pl.pallas_call(
        functools.partial(kernel, plan),
        in_specs=vmem(count) + [hbm] * len(outs),
        out_specs=[hbm, hbm] + vmem(len(loss)),
        out_shape=[pltpu.HBM((tokens, depth), BF16)] * 2 + loss,
        input_output_aliases={count + place: place for place in range(len(outs))},
        scratch_shapes=[
            pltpu.VMEM((tokens, depth), BF16),
            pltpu.VMEM((16 + extra, depth), BF16),
            pltpu.SemaphoreType.DMA((2 * depth // lane + 4,)),
        ],
        compiler_params=limit(6),
    )(*(near(part) for part in parts), *more, *outs)


def gather_kernel(plan, one, two, next_act, next_grad, wide, row, sems):
    def more(section, copy):
        if section == 0:
            wide[...] = jnp.zeros_like(wide)
            copy(wide, next_act)

    put_rows(plan, (one, two), (next_act, next_grad), row, sems, more)


def loss_rows_kernel(plan, part, grad, loss, _a, _g, next_act, next_grad, mean_loss, wide, row, sems):
    last = len(plan) - 1
    mean_loss[...] = jnp.where(lax.axis_index("section") == last, loss[...], 0.0)

    def more(section, copy):
        if section == last:
            wide[...] = jnp.broadcast_to(grad[...], wide.shape).astype(BF16)
            copy(wide, next_grad)

    put_rows(plan, (part,), (next_act, next_grad), row, sems, more)


def last_kernel(plan, part, _a, _g, next_act, next_grad, _wide, row, sems):
    put_rows(plan, (part,), (next_act, next_grad), row, sems, lambda *_: None)


def swap(value, axis, bit):
    count = lax.axis_size(axis)
    return lax.ppermute(value, axis, [(index, index ^ bit) for index in range(count)])


def local(
    activations,
    saved,
    cotangents,
    projection,
    section_gain,
    final_gain,
    head_weight,
    text_embed,
    labels,
):
    devices = lax.axis_size("dp")
    _, _, tokens, depth = activations.shape
    rows = head_weight.shape[0]
    act, kept, cot = (value.reshape(tokens, depth) for value in (activations, saved, cotangents))
    weight = projection[0]

    pack = pack_head(text_embed, head_weight)
    other = swap(pack, "section", 1)
    send_one, hand = early_block(act, kept, cot, section_gain, weight)
    one = swap(send_one, "section", 1)
    hand_high = swap(hand, "section", 2)
    pooled, send_three, send_two = later_block(act, kept, cot, section_gain, weight, hand)
    two = swap(send_two, "section", 1)
    pair = swap(stack(pack, other), "section", 2)
    packs = (pack, other, pair)
    text = own_text(packs, rows, depth)

    gain = final_gain.reshape(1, depth)
    table, standard = features(pooled, gain, labels)
    bit = 1
    while bit < devices:
        other = swap(table, "dp", bit)
        table = jnp.concatenate([table, other], axis=0)
        bit *= 2
    hand_low = swap(one, "section", 2)
    three = swap(choose(hand_high, send_three), "section", 1)
    mine, send = embed(table, text, packs, rows)
    bit = devices // 2
    while bit > 1:
        other = swap(send, "dp", bit)
        mine, send = fold(mine, other, bit, bit)
        bit //= 2
    other = swap(send, "dp", 1)
    grad, loss = loss_step(mine, other, table, standard, gain, tokens)
    plan = (
        ((1, 1, lane, True),),
        ((0, 0, 0, False), (1, 0, lane, True)),
        ((0, 1, 0, False), (1, 1, lane, True)),
        ((1, 0, lane, True),),
    )
    outs = rows_call(gather_kernel, plan, (one, two), (), tokens, depth)
    plan = ((), ((0, 1, 0, False),), ((0, 0, 0, False),), ())
    *outs, mean_loss = rows_call(
        loss_rows_kernel, plan, (hand_low,), (grad, loss), tokens, depth, outs
    )
    plan = (((0, 1, 0, False),), ((0, 1, lane, True),), ((0, 0, lane, True),), ((0, 0, 0, False),))
    next_act, next_grad = rows_call(last_kernel, plan, (three,), (), tokens, depth, outs)
    return (next_act[None, None], next_grad[None, None], mean_loss[0, 0:1])


def shifted(value, axis, steps):
    count = lax.axis_size(axis)
    first, last = (max(0, -steps), min(count, count - steps))
    return lax.ppermute(value, axis, [(source, source + steps) for source in range(first, last)])


def spread(block, axis, owner):
    block = jnp.where(lax.axis_index(axis) == owner, block, jnp.zeros_like(block))
    return lax.psum(block, axis)


def norm_rows(values):
    centre = jnp.mean(values, axis=-1, keepdims=True)
    centred = values - centre
    variance = jnp.mean(centred * centred, axis=-1, keepdims=True)
    inverse = lax.rsqrt(variance + epsilon)
    return (centred * inverse, inverse)


def unit_rows(values):
    inverse = lax.rsqrt(jnp.sum(values * values, axis=-1, keepdims=True) + epsilon)
    return (values * inverse, inverse)


def plain_forward(block_in, weight, scale_row):
    block_shape = block_in.shape
    standard, _ = norm_rows(block_in.astype(jnp.float32))
    normed = (standard * scale_row).astype(jnp.bfloat16)
    mixed = jnp.dot(normed.reshape(-1, block_shape[-1]), weight, preferred_element_type=jnp.float32)
    return (block_in.astype(jnp.float32) + mixed.reshape(block_shape)).astype(jnp.bfloat16)


def plain_backward(cotangent, restored, weight, scale_row):
    block_shape = restored.shape
    standard, inverse = norm_rows(restored.astype(jnp.float32))
    d_normed = lax.dot_general(
        cotangent.reshape(-1, block_shape[-1]),
        weight,
        (((1,), (1,)), ((), ())),
        preferred_element_type=jnp.float32,
    ).reshape(block_shape)
    d_standard = d_normed * scale_row
    d_input = cotangent.astype(jnp.float32) + inverse * (
        d_standard
        - jnp.mean(d_standard, axis=-1, keepdims=True)
        - standard * jnp.mean(d_standard * standard, axis=-1, keepdims=True)
    )
    return d_input.astype(jnp.bfloat16)


def contrastive(logits, label_values):
    count = logits.shape[0]
    targets = (label_values[:, None] == jnp.arange(count).astype(jnp.float32)[None, :]).astype(
        jnp.float32
    )
    row_lse = jax.nn.logsumexp(logits, axis=1)
    col_lse = jax.nn.logsumexp(logits, axis=0)
    picked = jnp.sum(logits * targets, axis=1)
    col_picked = jnp.sum(col_lse[None, :] * targets, axis=1)
    loss_value = 0.5 * jnp.mean(row_lse - picked) + 0.5 * jnp.mean(col_picked - picked)
    row_prob = jnp.exp(logits - row_lse[:, None])
    col_prob = jnp.exp(logits - col_lse[None, :])
    d_logits = 0.5 * (row_prob - targets + (col_prob - targets))
    return (loss_value, d_logits)


def plain_local(
    activations,
    saved,
    cotangents,
    projection,
    section_gain,
    final_gain,
    head_weight,
    text_embed,
    labels,
):
    sections = lax.axis_size("section")
    section_index = lax.axis_index("section")
    is_last = section_index == sections - 1
    weight = projection[0]
    scale_row = section_gain[0]
    incoming = activations[0]
    block_out = plain_forward(incoming, weight, scale_row)
    next_act = shifted(block_out[None], "section", 1)
    d_input = plain_backward(cotangents[0], saved[0], weight, scale_row)
    passed_grad = shifted(d_input[None], "section", -1)
    pooled = jnp.mean(block_out.astype(jnp.float32), axis=1)
    pooled_std, pooled_inv = norm_rows(pooled)
    pooled_norm = (pooled_std * final_gain).astype(jnp.bfloat16)
    shared = spread(pooled_norm, "section", sections - 1)
    row_count = head_weight.shape[0]
    my_columns = lax.dynamic_slice_in_dim(shared, section_index * row_count, row_count, 1)
    embedding = lax.psum(
        jnp.dot(my_columns, head_weight, preferred_element_type=jnp.float32), "section"
    )
    image_unit, image_inv = unit_rows(embedding)
    own_count = image_unit.shape[0]
    text_unit, _ = unit_rows(text_embed.astype(jnp.float32))
    all_image, all_text, all_labels = (
        lax.all_gather(image_unit, "dp", axis=0, tiled=True),
        lax.all_gather(text_unit, "dp", axis=0, tiled=True),
        lax.all_gather(labels.astype(jnp.float32), "dp", axis=0, tiled=True),
    )
    logits = logit_scale * jnp.dot(all_image, all_text.T, precision=lax.Precision.HIGHEST)
    loss_value, d_logits = contrastive(logits, all_labels)
    own_rows = lax.dynamic_slice_in_dim(d_logits, lax.axis_index("dp") * own_count, own_count, 0)
    d_image = logit_scale * jnp.dot(own_rows, all_text, precision=lax.Precision.HIGHEST)
    d_embedding = (
        (d_image - image_unit * jnp.sum(d_image * image_unit, axis=-1, keepdims=True)) * image_inv
    ).astype(jnp.bfloat16)
    partial_value = lax.dot_general(
        d_embedding, head_weight, (((1,), (1,)), ((), ())), preferred_element_type=jnp.float32
    )
    d_pooled_norm = lax.all_gather(partial_value, "section", axis=1, tiled=True)
    d_std = d_pooled_norm * final_gain
    d_pooled = pooled_inv * (
        d_std
        - jnp.mean(d_std, axis=-1, keepdims=True)
        - pooled_std * jnp.mean(d_std * pooled_std, axis=-1, keepdims=True)
    )
    token_count = block_out.shape[1]
    loss_grad = jnp.broadcast_to((d_pooled / token_count)[:, None, :], block_out.shape).astype(
        jnp.bfloat16
    )
    next_grad = jnp.where(is_last, loss_grad[None], passed_grad)
    mean_loss = jnp.where(is_last, loss_value, jnp.float32(0.0))[None]
    return (next_act, next_grad, mean_loss)


def fits(mesh, width, tokens):
    sections, devices = mesh.shape["section"], mesh.shape["dp"]
    power = devices > 1 and not (devices & (devices - 1))
    return sections == 4 and power and width == devices * lane and 0 < tokens - 2 * lane <= 8


def either(mesh, *args):
    if fits(mesh, args[7].shape[1], args[0].shape[2]):
        return local(*args)
    return plain_local(*args)


def solution(mesh):
    return jax.shard_map(
        functools.partial(either, mesh),
        mesh=mesh,
        in_specs=(
            P("section", "dp", None, None),
            P("section", "dp", None, None),
            P("section", "dp", None, None),
            P("section", None, None),
            P("section", None),
            P(),
            P("section", None),
            P("dp", None),
            P("dp"),
        ),
        out_specs=(P("section", "dp", None, None), P("section", "dp", None, None), P("section")),
        check_vma=False,
    )
```
